256 devices in a mesh: fsdp: 16 (over z, y_hi), cols: 16 (over y_lo, x, core).
Axes of the slice: x: 4, y: 4 (y_hi: 2, y_lo: 2; y = y_hi * 2 + y_lo), z: 8, core: 2. Of those that a mesh axis runs over, the one named last changes fastest.
Arguments:
- train_gate: bfloat16 [3584, 14336], P('fsdp', 'cols'), may hold values from -0.09375 to 0.09375
- low_gate: bfloat16 [3584, 16], P('fsdp'), may hold values from -0.09375 to 0.09375
- high_gate: bfloat16 [16, 14336], P(None, 'cols'), may hold values from -1.5 to 1.5
- train_up: bfloat16 [3584, 14336], P('fsdp', 'cols'), may hold values from -0.09375 to 0.09375
- low_up: bfloat16 [3584, 16], P('fsdp'), may hold values from -0.09375 to 0.09375
- high_up: bfloat16 [16, 14336], P(None, 'cols'), may hold values from -1.5 to 1.5
- train_down: bfloat16 [14336, 3584], P('cols', 'fsdp'), may hold values from -0.046875 to 0.046875
- low_down: bfloat16 [14336, 16], P('cols'), may hold values from -0.046875 to 0.046875
- high_down: bfloat16 [16, 3584], P(None, 'fsdp'), may hold values from -1.5 to 1.5
- norm_train: float32 [3584], P(('fsdp', 'cols')), may hold values from 0.25 to 1.75
- norm_step: float32 [3584], P(('fsdp', 'cols')), may hold values from -0.3 to 0.3
Outputs:
- serving_gate: bfloat16 [3584, 14336], P(None, 'cols')
- serving_up: bfloat16 [3584, 14336], P(None, 'cols')
- serving_down: bfloat16 [14336, 3584], P('cols')
- serve_norm: bfloat16 [3584], replicated
The draws below stay inside these ranges and needn't reach their ends.
All inputs are finite; a program needn't handle non-finite values.
Results may differ from the reference program's by a relative error of at most 0.001.
Values may be sent and summed in bfloat16 or wider, within the bound.
A program may use at most 128 MiB of HBM per device.

```python
import jax
import jax.numpy as jnp

D_MODEL = 3584
D_INNER = 14336
RANK = 16


def steps_of(stream_key, dims, shards, least, largest):
    factor_of = 1.0
    for position, shards_of in shards:
        heights = jax.random.uniform(jax.random.fold_in(jax.random.fold_in(stream_key, 6), position), (shards_of,), jnp.float32, least / len(shards), largest / len(shards))
        factor_of = factor_of * jnp.repeat(jnp.exp(heights), dims[position] // shards_of).reshape((-1,) + (1,) * (len(dims) - 1 - position))
    return factor_of


def gaussian(key, shape, width, reach, shards=(), dtype=jnp.bfloat16):
    entries = width * jax.random.normal(key, shape, jnp.float32)
    if shards:
        entries = entries * steps_of(key, shape, shards, -0.22, 0.18)
    return jnp.clip(entries, -reach, reach).astype(dtype)


def setup_inputs(seed: int = 0) -> dict:
    keys = jax.random.split(jax.random.key(seed), 12)
    return {
        "train_gate": gaussian(keys[0], (D_MODEL, D_INNER), D_MODEL ** -0.5, 0.09375, ((0, 16), (1, 16))),
        "low_gate": gaussian(keys[1], (D_MODEL, RANK), D_MODEL ** -0.5, 0.09375, ((0, 16),)),
        "high_gate": gaussian(keys[2], (RANK, D_INNER), RANK ** -0.5, 1.5, ((1, 16),)),
        "train_up": gaussian(keys[3], (D_MODEL, D_INNER), D_MODEL ** -0.5, 0.09375, ((0, 16), (1, 16))),
        "low_up": gaussian(keys[4], (D_MODEL, RANK), D_MODEL ** -0.5, 0.09375, ((0, 16),)),
        "high_up": gaussian(keys[5], (RANK, D_INNER), RANK ** -0.5, 1.5, ((1, 16),)),
        "train_down": gaussian(keys[6], (D_INNER, D_MODEL), D_INNER ** -0.5, 0.046875, ((0, 16), (1, 16))),
        "low_down": gaussian(keys[7], (D_INNER, RANK), D_INNER ** -0.5, 0.046875, ((0, 16),)),
        "high_down": gaussian(keys[8], (RANK, D_MODEL), RANK ** -0.5, 1.5, ((1, 16),)),
        "norm_train": jnp.clip(1.0 + 0.15 * jax.random.normal(keys[9], (D_MODEL,), jnp.float32), 0.25, 1.75),
        "norm_step": jnp.clip(jax.random.uniform(keys[10], (D_MODEL,), jnp.float32, -0.3, 0.3) * steps_of(keys[10], (D_MODEL,), ((0, 256),), -0.4, 0.0), -0.3, 0.3),
    }


mix_rate = 1.0


def reference(train_gate, low_gate, high_gate, train_up, low_up, high_up, train_down, low_down, high_down, norm_train, norm_step):
    whole_gate = train_gate.astype(jnp.float32) + mix_rate * jnp.dot(low_gate, high_gate, preferred_element_type=jnp.float32)
    whole_up = train_up.astype(jnp.float32) + mix_rate * jnp.dot(low_up, high_up, preferred_element_type=jnp.float32)
    whole_down = train_down.astype(jnp.float32) + mix_rate * jnp.dot(low_down, high_down, preferred_element_type=jnp.float32)
    serving_gate = whole_gate.astype(jnp.bfloat16)
    serving_up = whole_up.astype(jnp.bfloat16)
    serving_down = whole_down.astype(jnp.bfloat16)
    serve_norm = (norm_train + norm_step).astype(jnp.bfloat16)
    return serving_gate, serving_up, serving_down, serve_norm
```

```python
import functools

import jax
import jax.numpy as jnp
from jax import lax
from jax.experimental import pallas as pl
from jax.experimental.pallas import tpu as pltpu
from jax.sharding import PartitionSpec as P

MESH = pl.DeviceIdType.MESH
LANES = 128
DEPTH = 8
PIECES = 3
mix_rate = 1.0

ORDER = (
    (0, 0, 0, 0), (1, 0, 0, 0), (2, 0, 0, 0), (0, 0, 0, 1), (1, 0, 0, 2), (2, 0, 0, 2),
    (0, 0, 7, 0), (1, 0, 1, 0), (2, 0, 1, 0), (0, 1, 0, 0), (1, 0, 1, 2), (2, 0, 1, 2),
    (0, 0, 6, 0), (1, 0, 2, 0), (2, 0, 2, 0), (1, 0, 0, 1), (0, 1, 7, 0), (2, 0, 2, 2),
    (0, 1, 0, 2), (2, 0, 5, 0), (0, 0, 5, 0), (2, 0, 0, 1), (0, 0, 7, 1), (1, 1, 2, 0),
    (2, 0, 1, 1), (2, 0, 7, 1), (1, 1, 2, 2), (1, 1, 3, 0), (0, 1, 7, 2), (1, 1, 3, 2),
    (1, 0, 2, 2), (0, 0, 6, 1), (2, 0, 6, 1), (1, 1, 1, 1), (1, 0, 1, 1), (0, 1, 6, 2),
    (2, 1, 4, 2), (2, 1, 7, 2), (0, 1, 6, 1), (0, 0, 5, 1), (1, 1, 2, 1), (2, 1, 5, 2),
    (2, 1, 6, 2), (0, 1, 5, 1), (1, 0, 2, 1),
)
SLOTS = len(ORDER) // 3


def received(port, column, offset, piece):
    if port == 0:
        return column, (offset - 1) % DEPTH, piece
    if port == 1:
        return column, (offset + 1) % DEPTH, piece
    return 1 - column, offset, piece


def plan():
    arrives, slots, sends = {}, [0, 0, 0], []
    for port, *item in ORDER:
        arrives[received(port, *item)] = (port, slots[port])
        sends.append((port, slots[port], tuple(item)))
        slots[port] += 1
    return sends, arrives


def gather_kernel(n_fsdp, n_cols, *refs):
    bases, lows, highs = refs[0:3], refs[3:6], refs[6:9]
    norm_train, norm_step = refs[9:11]
    gates, ups, downs, serve_norm = refs[11:15]
    turned, base_vm, low_vm, high_down, high_gate, high_up, train_vm, step_vm, parts, groups = refs[15:25]
    send_sem, recv_sem, local_sem, col_send, col_recv, row_send, row_recv = refs[25:]
    high_vm = (high_down, high_gate, high_up)
    wholes = (turned, gates, ups)
    rows = base_vm.shape[1]
    here, col = lax.axis_index("fsdp"), lax.axis_index("cols")
    place, side = lax.div(here, 2), lax.rem(here, 2)

    loads = [
        pltpu.make_async_copy(src, dst, local_sem.at[s])
        for s, (src, dst) in enumerate(
            [p for c in range(PIECES) for p in ((bases[c], base_vm.at[c]), (lows[c], low_vm.at[c]), (highs[c], high_vm[c]))]
            + [(norm_train, train_vm), (norm_step, step_vm)]
        )
    ]
    for load in loads:
        load.start()

    barrier = pltpu.get_barrier_semaphore()
    for step in range(1, n_fsdp):
        peer = lax.rem(here + step, n_fsdp)
        pl.semaphore_signal(barrier, inc=1, device_id={"fsdp": peer}, device_id_type=MESH)
    for step in range(1, n_cols):
        peer = lax.rem(col + step, n_cols)
        pl.semaphore_signal(barrier, inc=1, device_id={"cols": peer}, device_id_type=MESH)

    def block_of(column, offset):
        return 2 * lax.rem(place + offset, DEPTH) + (side if column == 0 else 1 - side)

    def where(column, offset, piece):
        start = pl.multiple_of(block_of(column, offset) * rows, 32)
        return wholes[piece].at[pl.ds(start, rows)]

    def merge(c):
        for load in loads[3 * c : 3 * c + 3]:
            load.wait()
        product = lax.dot_general(
            low_vm[c], high_vm[c][...], (((0,), (0,)), ((), ())), preferred_element_type=jnp.float32
        )
        where(0, 0, c)[...] = (base_vm[c].astype(jnp.float32) + mix_rate * product).astype(jnp.bfloat16)

    sends, arrives = plan()
    targets = (2 * lax.rem(place + 1, DEPTH) + side, 2 * lax.rem(place + DEPTH - 1, DEPTH) + side, 2 * place + 1 - side)

    def copy(port, slot, item):
        return pltpu.make_async_remote_copy(
            src_ref=where(*item),
            dst_ref=where(*item),
            send_sem=send_sem.at[port, slot],
            recv_sem=recv_sem.at[port, slot],
            device_id={"fsdp": targets[port]},
            device_id_type=MESH,
        )

    held = set()

    def hold(item):
        if item in held:
            return
        held.add(item)
        if item[:2] == (0, 0):
            merge(item[2])
        else:
            port, slot = arrives[item]
            copy(port, slot, item).wait_recv()

    def turn(w):
        window = turned[LANES * w : LANES * (w + 1), :]
        downs[:, LANES * w : LANES * (w + 1)] = window.T

    def norm_copy(block, peer_axis, step):
        if peer_axis == "cols":
            size, ref, me, s, r = n_cols, parts, col, col_send, col_recv
        else:
            size, ref, me, s, r = n_fsdp, groups, here, row_send, row_recv
        return pltpu.make_async_remote_copy(
            src_ref=ref.at[me],
            dst_ref=ref.at[block],
            send_sem=s.at[step],
            recv_sem=r.at[step],
            device_id={peer_axis: lax.rem(me + step, size)},
            device_id_type=MESH,
        )

    length = train_vm.shape[0]
    span = n_cols * length

    def norm_first():
        loads[-2].wait()
        loads[-1].wait()
        flat = LANES * lax.broadcasted_iota(jnp.int32, (8, LANES), 0) + lax.broadcasted_iota(jnp.int32, (8, LANES), 1)
        first = lax.rem(here * span, LANES) + col * length
        tile = jnp.zeros((8, LANES), jnp.float32)
        for j in range(length):
            tile = jnp.where(flat == first + j, train_vm[j] + step_vm[j], tile)
        parts[col] = tile
        for step in range(1, n_cols):
            norm_copy(col, "cols", step).start()

    def norm_second():
        for step in range(1, n_cols):
            norm_copy(lax.rem(col + n_cols - step, n_cols), "cols", step).wait()
        total = parts[0]
        for c in range(1, n_cols):
            total = total + parts[c]
        groups[here] = total
        for step in range(1, n_fsdp):
            norm_copy(here, "fsdp", step).start()

    def norm_third():
        for step in range(1, n_fsdp):
            norm_copy(lax.rem(here + n_fsdp - step, n_fsdp), "fsdp", step).wait()
        lines = serve_norm.shape[0]
        out = [None] * lines
        for g in range(n_fsdp):
            line = g * span // LANES
            for r in range(-(-(g * span % LANES + span) // LANES)):
                value = groups[g, r : r + 1, :]
                out[line + r] = value if out[line + r] is None else out[line + r] + value
        serve_norm[...] = jnp.concatenate(out, axis=0).astype(serve_norm.dtype)

    hold((0, 0, 0))
    pl.semaphore_wait(barrier, n_fsdp - 1 + n_cols - 1)
    downs_in = [item for item in arrives if item[2] == 0]
    windows = list(range(n_fsdp * rows // LANES))
    ready = None
    for at, (port, slot, item) in enumerate(sends):
        hold(item)
        copy(port, slot, item).start()
        if at == 5:
            norm_first()
        if at == 12:
            norm_second()
        if at == 18:
            norm_third()
        if ready is None and at > 25 and all(i in held for i in downs_in):
            ready = at
        if at == 30:
            for i in downs_in:
                hold(i)
            ready = at
        if ready is not None:
            for w in windows[:2]:
                turn(w)
            del windows[:2]
    for w in windows:
        turn(w)
    for item in arrives:
        hold(item)
    for port, slot, item in sends:
        copy(port, slot, item).wait_send()


def gather(n_fsdp, n_cols, bases, lows, highs, norm_train, norm_step):
    rows, width = bases[0].shape
    rank = lows[0].shape[0]
    anywhere = pl.BlockSpec(memory_space=pl.ANY)
    inside = pl.BlockSpec(memory_space=pltpu.VMEM)
    dma = pltpu.SemaphoreType.DMA
    bf16, f32 = jnp.bfloat16, jnp.float32
    lines = n_fsdp * n_cols * norm_train.shape[0] // LANES
    return pl.pallas_call(
        functools.partial(gather_kernel, n_fsdp, n_cols),
        out_shape=[
            pltpu.VMEM((n_fsdp * rows, width), bf16),
            pltpu.VMEM((n_fsdp * rows, width), bf16),
            pltpu.VMEM((width, n_fsdp * rows), bf16),
            pltpu.VMEM((lines, LANES), bf16),
        ],
        in_specs=[anywhere] * 11,
        out_specs=[inside] * 4,
        scratch_shapes=[
            pltpu.VMEM((n_fsdp * rows, width), bf16),
            pltpu.VMEM((PIECES, rows, width), bf16),
            pltpu.VMEM((PIECES, rank, rows), bf16),
            pltpu.VMEM((rank, width), bf16),
            pltpu.VMEM((rank, width), bf16),
            pltpu.VMEM((rank, width), bf16),
            pltpu.SMEM(norm_train.shape, f32),
            pltpu.SMEM(norm_step.shape, f32),
            pltpu.VMEM((n_cols, 8, LANES), f32),
            pltpu.VMEM((n_fsdp, 8, LANES), f32),
            dma((3, SLOTS)),
            dma((3, SLOTS)),
            dma((3 * PIECES + 2,)),
            dma((n_cols,)),
            dma((n_cols,)),
            dma((n_fsdp,)),
            dma((n_fsdp,)),
        ],
        compiler_params=pltpu.CompilerParams(collective_id=0, has_side_effects=True, vmem_limit_bytes=42 * 2**20),
    )(*bases, *lows, *highs, norm_train, norm_step)


def write_kernel(*refs):
    ins, outs, sem = refs[:3], refs[3:6], refs[6]
    parts = sem.shape[1]
    copies = []
    for a in range(3):
        rows = ins[a].shape[0] // parts
        for p in range(parts):
            part = pl.ds(p * rows, rows)
            copies.append(pltpu.make_async_copy(ins[a].at[part], outs[a].at[part], sem.at[a, p]))
    for c in copies:
        c.start()
    for c in copies:
        c.wait()


def write(arrays):
    return pl.pallas_call(
        write_kernel,
        out_shape=[jax.ShapeDtypeStruct(a.shape, a.dtype) for a in arrays],
        in_specs=[pl.BlockSpec(memory_space=pltpu.VMEM)] * 3,
        out_specs=[pl.BlockSpec(memory_space=pl.ANY)] * 3,
        scratch_shapes=[pltpu.SemaphoreType.DMA((3, 4))],
        compiler_params=pltpu.CompilerParams(vmem_limit_bytes=8 * 2**20),
    )(*arrays)


def per_device(
    n_fsdp,
    n_cols,
    train_gate,
    low_gate,
    high_gate,
    train_up,
    low_up,
    high_up,
    train_down,
    low_down,
    high_down,
    norm_train,
    norm_step,
):
    gates, ups, downs, norm = gather(
        n_fsdp,
        n_cols,
        (train_down.T, train_gate, train_up),
        (high_down, low_gate.T, low_up.T),
        (low_down.T, high_gate, high_up),
        norm_train,
        norm_step,
    )
    gates, ups, downs = write((gates, ups, downs))
    return gates, ups, downs, norm.reshape(-1)


def solution(mesh):
    return jax.shard_map(
        functools.partial(per_device, mesh.shape["fsdp"], mesh.shape["cols"]),
        mesh=mesh,
        in_specs=(
            P("fsdp", "cols"),
            P("fsdp", None),
            P(None, "cols"),
            P("fsdp", "cols"),
            P("fsdp", None),
            P(None, "cols"),
            P("cols", "fsdp"),
            P("cols", None),
            P(None, "fsdp"),
            P(("fsdp", "cols")),
            P(("fsdp", "cols")),
        ),
        out_specs=(P(None, "cols"), P(None, "cols"), P("cols", None), P()),
        check_vma=False,
    )
```

```python
import functools

import jax
import jax.numpy as jnp
from jax import lax
from jax.experimental import pallas as pl
from jax.experimental.pallas import tpu as pltpu
from jax.sharding import PartitionSpec as P

MESH = pl.DeviceIdType.MESH
LANES = 128
DEPTH = 8
PIECES = 3
mix_rate = 1.0

ORDER = (
    (0, 0, 0, 0), (1, 0, 0, 0), (2, 0, 0, 0), (0, 0, 0, 1), (1, 0, 0, 2), (2, 0, 0, 2),
    (0, 0, 7, 0), (1, 0, 1, 0), (2, 0, 1, 0), (0, 1, 0, 0), (1, 0, 1, 2), (2, 0, 1, 2),
    (0, 0, 6, 0), (1, 0, 2, 0), (2, 0, 2, 0), (1, 0, 0, 1), (0, 1, 7, 0), (2, 0, 2, 2),
    (0, 1, 0, 2), (2, 0, 5, 0), (0, 0, 5, 0), (2, 0, 0, 1), (0, 0, 7, 1), (1, 1, 2, 0),
    (2, 0, 1, 1), (2, 0, 7, 1), (1, 1, 2, 2), (1, 1, 3, 0), (0, 1, 7, 2), (1, 1, 3, 2),
    (1, 0, 2, 2), (0, 0, 6, 1), (2, 0, 6, 1), (1, 1, 1, 1), (1, 0, 1, 1), (0, 1, 6, 2),
    (2, 1, 4, 2), (2, 1, 7, 2), (0, 1, 6, 1), (0, 0, 5, 1), (1, 1, 2, 1), (2, 1, 5, 2),
    (2, 1, 6, 2), (0, 1, 5, 1), (1, 0, 2, 1),
)
SLOTS = len(ORDER) // 3
NORM_AT = (6, 8, 10, 12)
WRITES = 4


def received(port, column, offset, piece):
    if port == 0:
        return column, (offset - 1) % DEPTH, piece
    if port == 1:
        return column, (offset + 1) % DEPTH, piece
    return 1 - column, offset, piece


def plan():
    arrives, slots, sends = {}, [0, 0, 0], []
    for port, *item in ORDER:
        arrives[received(port, *item)] = (port, slots[port])
        sends.append((port, slots[port], tuple(item)))
        slots[port] += 1
    return sends, arrives


def partners_of(col):
    core, x, y = lax.rem(col, 2), lax.rem(lax.div(col, 2), 4), lax.div(col, 8)
    odd = lax.rem(x, 2)

    def at(y, x, core):
        return (4 * y + x) * 2 + core

    return (
        at(y, x, 1 - core),
        at(y, x + 1 - 2 * odd, core),
        at(y, lax.rem(x + 3 + 2 * odd, 4), core),
        at(1 - y, x, core),
    )


def gather_kernel(n_fsdp, n_cols, *refs):
    bases, lows, highs = refs[0:3], refs[3:6], refs[6:9]
    norm_train, norm_step = refs[9:11]
    gates, ups, downs, serve_norm = refs[11:15]
    turned, base_vm, low_vm, high_down, high_gate, high_up, train_vm, step_vm, sums, parts, groups = refs[15:26]
    send_sem, recv_sem, local_sem, col_send, col_recv, row_send, row_recv = refs[26:]
    high_vm = (high_down, high_gate, high_up)
    wholes = (turned, gates, ups)
    rows = base_vm.shape[1]
    here, col = lax.axis_index("fsdp"), lax.axis_index("cols")
    place, side = lax.div(here, 2), lax.rem(here, 2)

    loads = [
        pltpu.make_async_copy(src, dst, local_sem.at[s])
        for s, (src, dst) in enumerate(
            [p for c in range(PIECES) for p in ((bases[c], base_vm.at[c]), (lows[c], low_vm.at[c]), (highs[c], high_vm[c]))]
            + [(norm_train, train_vm), (norm_step, step_vm)]
        )
    ]
    for load in loads:
        load.start()

    barrier = pltpu.get_barrier_semaphore()
    targets = (2 * lax.rem(place + 1, DEPTH) + side, 2 * lax.rem(place + DEPTH - 1, DEPTH) + side, 2 * place + 1 - side)
    for peer in targets:
        pl.semaphore_signal(barrier, inc=1, device_id={"fsdp": peer}, device_id_type=MESH)
    partners = partners_of(col)
    for peer in partners:
        pl.semaphore_signal(barrier, inc=1, device_id={"cols": peer}, device_id_type=MESH)

    def block_of(column, offset):
        return 2 * lax.rem(place + offset, DEPTH) + (side if column == 0 else 1 - side)

    def where(column, offset, piece):
        start = pl.multiple_of(block_of(column, offset) * rows, 32)
        return wholes[piece].at[pl.ds(start, rows)]

    def merge(c):
        for load in loads[3 * c : 3 * c + 3]:
            load.wait()
        product = lax.dot_general(
            low_vm[c], high_vm[c][...], (((0,), (0,)), ((), ())), preferred_element_type=jnp.float32
        )
        where(0, 0, c)[...] = (base_vm[c].astype(jnp.float32) + mix_rate * product).astype(jnp.bfloat16)

    sends, arrives = plan()

    def copy(port, slot, item):
        return pltpu.make_async_remote_copy(
            src_ref=where(*item),
            dst_ref=where(*item),
            send_sem=send_sem.at[port, slot],
            recv_sem=recv_sem.at[port, slot],
            device_id={"fsdp": targets[port]},
            device_id_type=MESH,
        )

    held = set()

    def hold(item):
        if item in held:
            return
        held.add(item)
        if item[:2] == (0, 0):
            merge(item[2])
        else:
            port, slot = arrives[item]
            copy(port, slot, item).wait_recv()

    def turn(w):
        window = turned[LANES * w : LANES * (w + 1), :]
        downs[:, LANES * w : LANES * (w + 1)] = window.T

    length = train_vm.shape[0]
    span = n_cols * length
    tall = -(-(span + LANES - 1) // LANES)

    def exchange(step):
        return pltpu.make_async_remote_copy(
            src_ref=sums.at[step, pl.ds(0, tall)],
            dst_ref=parts.at[step, pl.ds(0, tall)],
            send_sem=col_send.at[step],
            recv_sem=col_recv.at[step],
            device_id={"cols": partners[step]},
            device_id_type=MESH,
        )

    def norm_step_at(step):
        if step == 0:
            loads[-2].wait()
            loads[-1].wait()
            flat = LANES * lax.broadcasted_iota(jnp.int32, (8, LANES), 0) + lax.broadcasted_iota(jnp.int32, (8, LANES), 1)
            first = lax.rem(here * span, LANES) + col * length
            tile = jnp.zeros((8, LANES), jnp.float32)
            for j in range(length):
                tile = jnp.where(flat == first + j, train_vm[j] + step_vm[j], tile)
            sums[0] = tile
        else:
            exchange(step - 1).wait()
            sums[step, 0:tall] = sums[step - 1, 0:tall] + parts[step - 1, 0:tall]
        exchange(step).start()

    def norm_copy(block, step):
        return pltpu.make_async_remote_copy(
            src_ref=groups.at[here, pl.ds(0, tall)],
            dst_ref=groups.at[block, pl.ds(0, tall)],
            send_sem=row_send.at[step],
            recv_sem=row_recv.at[step],
            device_id={"fsdp": lax.rem(here + step, n_fsdp)},
            device_id_type=MESH,
        )

    def norm_spread():
        exchange(3).wait()
        groups[here, 0:tall] = sums[3, 0:tall] + parts[3, 0:tall]
        for step in range(1, n_fsdp):
            norm_copy(here, step).start()

    def norm_last():
        for step in range(1, n_fsdp):
            norm_copy(lax.rem(here + n_fsdp - step, n_fsdp), step).wait()
        lines = serve_norm.shape[0]
        out = [None] * lines
        for g in range(n_fsdp):
            line = g * span // LANES
            for r in range(-(-(g * span % LANES + span) // LANES)):
                value = groups[g, r : r + 1, :]
                out[line + r] = value if out[line + r] is None else out[line + r] + value
        serve_norm[...] = jnp.concatenate(out, axis=0).astype(serve_norm.dtype)

    hold((0, 0, 0))
    pl.semaphore_wait(barrier, len(targets) + len(partners))
    downs_in = [item for item in arrives if item[2] == 0]
    windows = list(range(n_fsdp * rows // LANES))
    ready = None
    for at, (port, slot, item) in enumerate(sends):
        hold(item)
        copy(port, slot, item).start()
        if at in NORM_AT:
            norm_step_at(NORM_AT.index(at))
        if at == 30:
            for i in downs_in:
                hold(i)
            ready = at
            norm_spread()
        if at == 43:
            norm_last()
        if ready is not None:
            for w in windows[:2]:
                turn(w)
            del windows[:2]
    for w in windows:
        turn(w)
    for item in arrives:
        hold(item)
    for port, slot, item in sends:
        copy(port, slot, item).wait_send()


def gather(n_fsdp, n_cols, bases, lows, highs, norm_train, norm_step):
    rows, width = bases[0].shape
    rank = lows[0].shape[0]
    anywhere = pl.BlockSpec(memory_space=pl.ANY)
    inside = pl.BlockSpec(memory_space=pltpu.VMEM)
    dma = pltpu.SemaphoreType.DMA
    bf16, f32 = jnp.bfloat16, jnp.float32
    lines = n_fsdp * n_cols * norm_train.shape[0] // LANES
    return pl.pallas_call(
        functools.partial(gather_kernel, n_fsdp, n_cols),
        out_shape=[
            pltpu.VMEM((n_fsdp * rows, width), bf16),
            pltpu.VMEM((n_fsdp * rows, width), bf16),
            pltpu.VMEM((width, n_fsdp * rows), bf16),
            pltpu.VMEM((lines, LANES), bf16),
        ],
        in_specs=[anywhere] * 11,
        out_specs=[inside] * 4,
        scratch_shapes=[
            pltpu.VMEM((n_fsdp * rows, width), bf16),
            pltpu.VMEM((PIECES, rows, width), bf16),
            pltpu.VMEM((PIECES, rank, rows), bf16),
            pltpu.VMEM((rank, width), bf16),
            pltpu.VMEM((rank, width), bf16),
            pltpu.VMEM((rank, width), bf16),
            pltpu.SMEM(norm_train.shape, f32),
            pltpu.SMEM(norm_step.shape, f32),
            pltpu.VMEM((4, 8, LANES), f32),
            pltpu.VMEM((4, 8, LANES), f32),
            pltpu.VMEM((n_fsdp, 8, LANES), f32),
            dma((3, SLOTS)),
            dma((3, SLOTS)),
            dma((3 * PIECES + 2,)),
            dma((4,)),
            dma((4,)),
            dma((n_fsdp,)),
            dma((n_fsdp,)),
        ],
        compiler_params=pltpu.CompilerParams(collective_id=0, has_side_effects=True, vmem_limit_bytes=42 * 2**20),
    )(*bases, *lows, *highs, norm_train, norm_step)


def write_kernel(*refs):
    ins, outs, sem = refs[:4], refs[4:8], refs[8]
    parts = sem.shape[1]
    copies = [pltpu.make_async_copy(ins[3], outs[3], sem.at[3, 0])]
    for p in range(parts):
        for a in range(3):
            rows = ins[a].shape[0] // parts
            part = pl.ds(p * rows, rows)
            copies.append(pltpu.make_async_copy(ins[a].at[part], outs[a].at[part], sem.at[a, p]))
    for c in copies:
        c.start()
    for c in copies:
        c.wait()


def write(arrays):
    return pl.pallas_call(
        write_kernel,
        out_shape=[jax.ShapeDtypeStruct(a.shape, a.dtype) for a in arrays],
        in_specs=[pl.BlockSpec(memory_space=pltpu.VMEM)] * 4,
        out_specs=[pl.BlockSpec(memory_space=pl.ANY)] * 4,
        scratch_shapes=[pltpu.SemaphoreType.DMA((4, WRITES))],
        compiler_params=pltpu.CompilerParams(vmem_limit_bytes=8 * 2**20),
    )(*arrays)


def per_device(
    n_fsdp,
    n_cols,
    train_gate,
    low_gate,
    high_gate,
    train_up,
    low_up,
    high_up,
    train_down,
    low_down,
    high_down,
    norm_train,
    norm_step,
):
    gates, ups, downs, norm = gather(
        n_fsdp,
        n_cols,
        (train_down.T, train_gate, train_up),
        (high_down, low_gate.T, low_up.T),
        (low_down.T, high_gate, high_up),
        norm_train,
        norm_step,
    )
    gates, ups, downs, norm = write((gates, ups, downs, norm))
    return gates, ups, downs, norm.reshape(-1)


def solution(mesh):
    return jax.shard_map(
        functools.partial(per_device, mesh.shape["fsdp"], mesh.shape["cols"]),
        mesh=mesh,
        in_specs=(
            P("fsdp", "cols"),
            P("fsdp", None),
            P(None, "cols"),
            P("fsdp", "cols"),
            P("fsdp", None),
            P(None, "cols"),
            P("cols", "fsdp"),
            P("cols", None),
            P(None, "fsdp"),
            P(("fsdp", "cols")),
            P(("fsdp", "cols")),
        ),
        out_specs=(P(None, "cols"), P(None, "cols"), P("cols", None), P()),
        check_vma=False,
    )
```

```python
import functools

import jax
import jax.numpy as jnp
from jax import lax
from jax.experimental import pallas as pl
from jax.experimental.pallas import tpu as pltpu
from jax.sharding import PartitionSpec as P

MESH = pl.DeviceIdType.MESH
LANES = 128
DEPTH = 8
mix_rate = 1.0

WHOLE = (
    (0, 0, 0, 0), (1, 0, 0, 0), (2, 0, 0, 0), (0, 0, 0, 1), (1, 0, 0, 2), (2, 0, 0, 2),
    (0, 0, 7, 0), (1, 0, 1, 0), (2, 0, 1, 0), (0, 1, 0, 0), (1, 0, 1, 2), (2, 0, 1, 2),
    (0, 0, 6, 0), (1, 0, 2, 0), (2, 0, 2, 0), (1, 0, 0, 1), (0, 1, 7, 0), (2, 0, 2, 2),
    (0, 1, 0, 2), (2, 0, 5, 0), (0, 0, 5, 0), (2, 0, 0, 1), (0, 0, 7, 1), (1, 1, 2, 0),
    (2, 0, 1, 1), (2, 0, 7, 1), (1, 1, 2, 2), (1, 1, 3, 0), (0, 1, 7, 2), (1, 1, 3, 2),
    (1, 0, 2, 2), (0, 0, 6, 1), (2, 0, 6, 1), (1, 1, 1, 1), (1, 0, 1, 1), (0, 1, 6, 2),
    (2, 1, 4, 2), (2, 1, 7, 2), (0, 1, 6, 1), (0, 0, 5, 1), (1, 1, 2, 1), (2, 1, 5, 2),
    (2, 1, 6, 2), (0, 1, 5, 1), (1, 0, 2, 1),
)
FIRST = (
    (0, 0, 0, 0), (1, 0, 0, 0), (2, 0, 0, 0), (0, 0, 0, 1), (1, 0, 0, 1), (2, 0, 0, 1),
    (0, 0, 7, 0), (1, 0, 1, 0), (2, 0, 1, 0), (2, 0, 7, 0), (0, 0, 7, 1), (1, 0, 1, 1),
    (0, 0, 6, 0), (2, 0, 6, 0), (1, 1, 1, 0), (1, 0, 2, 0), (0, 0, 6, 1), (2, 0, 6, 1),
    (0, 0, 5, 0), (1, 1, 2, 0), (2, 0, 5, 0), (1, 0, 2, 1), (2, 0, 2, 1), (1, 1, 0, 1),
    (2, 0, 7, 1), (0, 1, 6, 1), (0, 1, 5, 0), (0, 1, 5, 1), (1, 0, 3, 1), (2, 0, 3, 1),
)
SECOND = (
    (0, 0, 0, 1), (1, 0, 0, 0), (2, 0, 0, 1), (0, 0, 0, 0), (1, 0, 0, 1), (2, 0, 0, 0),
    (0, 0, 7, 1), (1, 0, 1, 0), (2, 0, 7, 1), (1, 1, 0, 1), (0, 0, 7, 0), (2, 0, 7, 0),
    (1, 1, 0, 0), (0, 0, 6, 1), (2, 0, 6, 1), (1, 0, 2, 0), (2, 0, 2, 0), (0, 0, 6, 0),
    (1, 1, 1, 1), (2, 0, 6, 0), (1, 0, 1, 1), (0, 0, 5, 1), (2, 0, 3, 0), (2, 0, 5, 1),
    (0, 0, 5, 0), (1, 1, 2, 1), (0, 0, 4, 1), (2, 0, 4, 1), (0, 1, 6, 0), (1, 1, 3, 0),
)
NORM_AT = (8, 10, 12)


def received(port, column, offset, chunk):
    if port == 0:
        return column, (offset - 1) % DEPTH, chunk
    if port == 1:
        return column, (offset + 1) % DEPTH, chunk
    return 1 - column, offset, chunk


def plan(order):
    arrives, slots, sends = {}, [0, 0, 0], []
    for port, *item in order:
        arrives[received(port, *item)] = (port, slots[port])
        sends.append((port, slots[port], tuple(item)))
        slots[port] += 1
    return sends, arrives


def partners_of(col):
    core, x, y = lax.rem(col, 2), lax.rem(lax.div(col, 2), 4), lax.div(col, 8)
    odd = lax.rem(x, 2)

    def at(y, x, core):
        return (4 * y + x) * 2 + core

    return (
        at(y, x, 1 - core),
        at(y, x + 1 - 2 * odd, core),
        at(y, lax.rem(x + 3 + 2 * odd, 4), core),
        at(1 - y, x, core),
    )


def targets_of(here):
    place, side = lax.div(here, 2), lax.rem(here, 2)
    return (
        2 * lax.rem(place + 1, DEPTH) + side,
        2 * lax.rem(place + DEPTH - 1, DEPTH) + side,
        2 * place + 1 - side,
    )


class Exchange:
    def __init__(self, order, bases, lows, highs, base_vm, low_vm, high_vm, wholes, send_sem, recv_sem, load_sem):
        self.sends, self.arrives = plan(order)
        self.wholes, self.base_vm, self.low_vm, self.high_vm = wholes, base_vm, low_vm, high_vm
        self.send_sem, self.recv_sem = send_sem, recv_sem
        self.rows = base_vm.shape[1]
        self.parts = (max(item[2] for item in self.arrives) + 1) // len(wholes)
        here = lax.axis_index("fsdp")
        self.place, self.side = lax.div(here, 2), lax.rem(here, 2)
        self.targets = targets_of(here)
        self.held = set()
        self.merged = set()
        self.loads = []
        for c in range(len(wholes)):
            for n, (src, dst) in enumerate(((bases[c], base_vm.at[c]), (lows[c], low_vm.at[c]), (highs[c], high_vm.at[c]))):
                self.loads.append(pltpu.make_async_copy(src, dst, load_sem.at[c, n]))
        for load in self.loads:
            load.start()

    def where(self, column, offset, chunk):
        size = self.rows // self.parts
        block = 2 * lax.rem(self.place + offset, DEPTH) + (self.side if column == 0 else 1 - self.side)
        start = pl.multiple_of(block * self.rows + chunk % self.parts * size, 16)
        return self.wholes[chunk // self.parts].at[pl.ds(start, size)]

    def merge(self, c):
        if c in self.merged:
            return
        self.merged.add(c)
        for load in self.loads[3 * c : 3 * c + 3]:
            load.wait()
        product = lax.dot_general(
            self.low_vm[c], self.high_vm[c], (((0,), (0,)), ((), ())), preferred_element_type=jnp.float32
        )
        value = (self.base_vm[c].astype(jnp.float32) + mix_rate * product).astype(jnp.bfloat16)
        start = pl.multiple_of((2 * self.place + self.side) * self.rows, 16)
        self.wholes[c][pl.ds(start, self.rows), :] = value

    def copy(self, port, slot, item):
        return pltpu.make_async_remote_copy(
            src_ref=self.where(*item),
            dst_ref=self.where(*item),
            send_sem=self.send_sem.at[port, slot],
            recv_sem=self.recv_sem.at[port, slot],
            device_id={"fsdp": self.targets[port]},
            device_id_type=MESH,
        )

    def hold(self, item):
        if item in self.held:
            return
        self.held.add(item)
        if item[:2] == (0, 0):
            self.merge(item[2] // self.parts)
        else:
            port, slot = self.arrives[item]
            self.copy(port, slot, item).wait_recv()

    def send(self, at):
        port, slot, item = self.sends[at]
        self.hold(item)
        self.copy(port, slot, item).start()

    def finish(self):
        for item in self.arrives:
            self.hold(item)
        for port, slot, item in self.sends:
            self.copy(port, slot, item).wait_send()


def norm_spread(groups, tall, row_send, row_recv, outward):
    here, n_fsdp = lax.axis_index("fsdp"), groups.shape[0]

    def norm_copy(block, step):
        return pltpu.make_async_remote_copy(
            src_ref=groups.at[here, pl.ds(0, tall)],
            dst_ref=groups.at[block, pl.ds(0, tall)],
            send_sem=row_send.at[step],
            recv_sem=row_recv.at[step],
            device_id={"fsdp": lax.rem(here + step, n_fsdp)},
            device_id_type=MESH,
        )

    if outward:
        return [norm_copy(here, step) for step in range(1, n_fsdp)]
    return [norm_copy(lax.rem(here + n_fsdp - step, n_fsdp), step) for step in range(1, n_fsdp)]


def norm_lines(groups, span, serve_norm):
    out = [None] * serve_norm.shape[0]
    for g in range(groups.shape[0]):
        line = g * span // LANES
        for r in range(-(-(g * span % LANES + span) // LANES)):
            value = groups[g, r : r + 1, :]
            out[line + r] = value if out[line + r] is None else out[line + r] + value
    serve_norm[...] = jnp.concatenate(out, axis=0).astype(serve_norm.dtype)


def first_kernel(n_fsdp, n_cols, *refs):
    bases, lows, highs = refs[0:3], refs[3:6], refs[6:9]
    norm_train, norm_step = refs[9:11]
    gates, ups, downs, group, serve_norm = refs[11:16]
    turned, base_vm, low_vm, high_vm, train_vm, step_vm, sums, parts, groups = refs[16:25]
    send_sem, recv_sem, load_sem, norm_sem, col_send, col_recv, row_send, row_recv = refs[25:]
    here, col = lax.axis_index("fsdp"), lax.axis_index("cols")
    core = lax.rem(col, 2)

    def start_exchange(order, count):
        return Exchange(
            order, bases[:count], lows[:count], highs[:count], base_vm, low_vm, high_vm, (turned, gates, ups)[:count],
            send_sem, recv_sem, load_sem,
        )

    norm_loads = [
        pltpu.make_async_copy(norm_train, train_vm, norm_sem.at[0]),
        pltpu.make_async_copy(norm_step, step_vm, norm_sem.at[1]),
    ]
    barrier = pltpu.get_barrier_semaphore()
    targets, partners = targets_of(here), partners_of(col)
    for peer in targets:
        pl.semaphore_signal(barrier, inc=1, device_id={"fsdp": peer}, device_id_type=MESH)
    for peer in partners:
        pl.semaphore_signal(barrier, inc=1, device_id={"cols": peer}, device_id_type=MESH)

    length = train_vm.shape[0]
    span = n_cols * length
    tall = -(-(span + LANES - 1) // LANES)

    def exchange(step):
        return pltpu.make_async_remote_copy(
            src_ref=sums.at[step, pl.ds(0, tall)],
            dst_ref=parts.at[step, pl.ds(0, tall)],
            send_sem=col_send.at[step],
            recv_sem=col_recv.at[step],
            device_id={"cols": partners[step]},
            device_id_type=MESH,
        )

    def norm_begin():
        for load in norm_loads:
            load.wait()
        flat = LANES * lax.broadcasted_iota(jnp.int32, (8, LANES), 0) + lax.broadcasted_iota(jnp.int32, (8, LANES), 1)
        first = lax.rem(here * span, LANES) + col * length
        tile = jnp.zeros((8, LANES), jnp.float32)
        for j in range(length):
            tile = jnp.where(flat == first + j, train_vm[j] + step_vm[j], tile)
        sums[0] = tile
        exchange(0).start()

    def norm_go_on(step):
        exchange(step - 1).wait()
        sums[step, 0:tall] = sums[step - 1, 0:tall] + parts[step - 1, 0:tall]
        exchange(step).start()

    def turn(x, at, windows):
        for item in x.arrives:
            if item[2] == 0:
                x.hold(item)
        for w in windows:
            downs[:, LANES * w : LANES * (w + 1)] = turned[LANES * w : LANES * (w + 1), :].T

    windows = range(turned.shape[0] // LANES)

    @pl.when(core == 0)
    def _():
        x = start_exchange(WHOLE, 3)
        for load in norm_loads:
            load.start()
        x.merge(0)
        pl.semaphore_wait(barrier, len(targets) + len(partners))
        for at in range(len(x.sends)):
            x.send(at)
            if at == 5:
                norm_begin()
            if at in NORM_AT:
                norm_go_on(NORM_AT.index(at) + 1)
            if at == 30:
                turn(x, at, ())
                exchange(3).wait()
                groups[here, 0:tall] = sums[3, 0:tall] + parts[3, 0:tall]
                for copy in norm_spread(groups, tall, row_send, row_recv, True):
                    copy.start()
            if at > 30:
                turn(x, at, windows[2 * (at - 31) : 2 * (at - 30)])
            if at == 43:
                for copy in norm_spread(groups, tall, row_send, row_recv, False):
                    copy.wait()
                norm_lines(groups, span, serve_norm)
        turn(x, at, windows[2 * (len(x.sends) - 31) :])
        x.finish()

    @pl.when(core == 1)
    def _():
        x = start_exchange(FIRST, 2)
        for load in norm_loads:
            load.start()
        x.merge(0)
        pl.semaphore_wait(barrier, len(targets) + len(partners))
        for at in range(len(x.sends)):
            x.send(at)
            if at == 5:
                norm_begin()
            if at in NORM_AT:
                norm_go_on(NORM_AT.index(at) + 1)
        exchange(3).wait()
        group[...] = jnp.zeros_like(group)
        group[0:tall] = sums[3, 0:tall] + parts[3, 0:tall]
        turn(x, at, windows)
        x.finish()


def second_kernel(n_fsdp, n_cols, length, *refs):
    bases, lows, highs, group = refs[0:1], refs[1:2], refs[2:3], refs[3]
    ups, serve_norm = refs[4:6]
    base_vm, low_vm, high_vm, groups = refs[6:10]
    send_sem, recv_sem, load_sem, row_send, row_recv = refs[10:]
    here, col = lax.axis_index("fsdp"), lax.axis_index("cols")
    barrier = pltpu.get_barrier_semaphore()
    targets = targets_of(here)
    span = n_cols * length
    tall = -(-(span + LANES - 1) // LANES)

    @pl.when(lax.rem(col, 2) == 1)
    def _():
        for peer in targets:
            pl.semaphore_signal(barrier, inc=1, device_id={"fsdp": peer}, device_id_type=MESH)
        x = Exchange(SECOND, bases, lows, highs, base_vm, low_vm, high_vm, (ups,), send_sem, recv_sem, load_sem)
        groups[here] = group[...]
        x.merge(0)
        pl.semaphore_wait(barrier, len(targets))
        place, side = lax.div(here, 2), lax.rem(here, 2)

        def across(block):
            return pltpu.make_async_remote_copy(
                src_ref=groups.at[here, pl.ds(0, tall)],
                dst_ref=groups.at[block, pl.ds(0, tall)],
                send_sem=row_send.at[0],
                recv_sem=row_recv.at[0],
                device_id={"fsdp": targets[2]},
                device_id_type=MESH,
            )

        def along(first, step):
            return pltpu.make_async_remote_copy(
                src_ref=groups.at[pl.ds(2 * place, 2), pl.ds(0, tall)],
                dst_ref=groups.at[pl.ds(2 * first, 2), pl.ds(0, tall)],
                send_sem=row_send.at[step],
                recv_sem=row_recv.at[step],
                device_id={"fsdp": 2 * lax.rem(place + step, DEPTH) + side},
                device_id_type=MESH,
            )

        across(here).start()
        for at in range(len(x.sends)):
            x.send(at)
            if at == len(x.sends) - 3:
                for o in range(1, DEPTH):
                    x.hold(next(i for i in [t[2] for t in x.sends] + list(x.arrives) if i[:2] == (0, o) and i in x.arrives))
                across(2 * place + 1 - side).wait()
                for step in range(1, DEPTH):
                    along(place, step).start()
        x.finish()
        for step in range(1, DEPTH):
            along(lax.rem(place + DEPTH - step, DEPTH), step).wait()
        norm_lines(groups, span, serve_norm)


ANYWHERE = pl.BlockSpec(memory_space=pl.ANY)
INSIDE = pl.BlockSpec(memory_space=pltpu.VMEM)
DMA = pltpu.SemaphoreType.DMA
MIB = 2**20
PARTS = 4


def first(n_fsdp, n_cols, bases, lows, highs, norm_train, norm_step):
    rows, width = bases[0].shape
    rank = lows[0].shape[0]
    bf16, f32 = jnp.bfloat16, jnp.float32
    slots = len(WHOLE) // 3
    return pl.pallas_call(
        functools.partial(first_kernel, n_fsdp, n_cols),
        out_shape=[
            pltpu.VMEM((n_fsdp * rows, width), bf16),
            pltpu.VMEM((n_fsdp * rows, width), bf16),
            pltpu.VMEM((width, n_fsdp * rows), bf16),
            pltpu.VMEM((8, LANES), f32),
            pltpu.VMEM((n_fsdp * n_cols * norm_train.shape[0] // LANES, LANES), bf16),
        ],
        in_specs=[ANYWHERE] * 11,
        out_specs=[INSIDE] * 5,
        scratch_shapes=[
            pltpu.VMEM((n_fsdp * rows, width), bf16),
            pltpu.VMEM((3, rows, width), bf16),
            pltpu.VMEM((3, rank, rows), bf16),
            pltpu.VMEM((3, rank, width), bf16),
            pltpu.SMEM(norm_train.shape, f32),
            pltpu.SMEM(norm_step.shape, f32),
            pltpu.VMEM((4, 8, LANES), f32),
            pltpu.VMEM((4, 8, LANES), f32),
            pltpu.VMEM((n_fsdp, 8, LANES), f32),
            DMA((3, slots)),
            DMA((3, slots)),
            DMA((3, 3)),
            DMA((2,)),
            DMA((4,)),
            DMA((4,)),
            DMA((n_fsdp,)),
            DMA((n_fsdp,)),
        ],
        compiler_params=pltpu.CompilerParams(collective_id=0, has_side_effects=True, vmem_limit_bytes=42 * MIB),
    )(*bases, *lows, *highs, norm_train, norm_step)


def second(n_fsdp, n_cols, length, base, low, high, group):
    rows, width = base.shape
    rank = low.shape[0]
    bf16, f32 = jnp.bfloat16, jnp.float32
    slots = len(SECOND) // 3
    return pl.pallas_call(
        functools.partial(second_kernel, n_fsdp, n_cols, length),
        out_shape=[
            pltpu.VMEM((n_fsdp * rows, width), bf16),
            pltpu.VMEM((n_fsdp * n_cols * length // LANES, LANES), bf16),
        ],
        in_specs=[ANYWHERE] * 3 + [INSIDE],
        out_specs=[INSIDE] * 2,
        scratch_shapes=[
            pltpu.VMEM((1, rows, width), bf16),
            pltpu.VMEM((1, rank, rows), bf16),
            pltpu.VMEM((1, rank, width), bf16),
            pltpu.VMEM((n_fsdp, 8, LANES), f32),
            DMA((3, slots)),
            DMA((3, slots)),
            DMA((1, 3)),
            DMA((n_fsdp,)),
            DMA((n_fsdp,)),
        ],
        compiler_params=pltpu.CompilerParams(collective_id=1, has_side_effects=True, vmem_limit_bytes=50 * MIB),
    )(base, low, high, group)


def run_copies(refs, sem):
    copies = []
    for a, (src, dst, parts) in enumerate(refs):
        rows = src.shape[0] // parts
        for p in range(parts):
            part = pl.ds(p * rows, rows)
            copies.append(pltpu.make_async_copy(src.at[part], dst.at[part], sem.at[a, p]))
    for c in copies:
        c.start()
    for c in copies:
        c.wait()


def write_first_kernel(gates, ups, downs, norm, group, gates_out, ups_out, downs_out, norm_out, group_out, sem):
    core = lax.rem(lax.axis_index("cols"), 2)
    group_out[...] = group[...]
    both = [(gates, gates_out, PARTS), (downs, downs_out, PARTS)]

    @pl.when(core == 0)
    def _():
        run_copies(both + [(ups, ups_out, PARTS), (norm, norm_out, 1)], sem)

    @pl.when(core == 1)
    def _():
        run_copies(both, sem)


def write_first(gates, ups, downs, norm, group):
    arrays = (gates, ups, downs, norm)
    return pl.pallas_call(
        write_first_kernel,
        out_shape=[jax.ShapeDtypeStruct(a.shape, a.dtype) for a in arrays] + [pltpu.VMEM(group.shape, group.dtype)],
        in_specs=[INSIDE] * 5,
        out_specs=[ANYWHERE] * 4 + [INSIDE],
        scratch_shapes=[DMA((4, PARTS))],
        compiler_params=pltpu.CompilerParams(vmem_limit_bytes=8 * MIB),
    )(*arrays, group)


def write_second_kernel(ups, norm, ups_in, norm_in, ups_out, norm_out, sem):
    del ups_in, norm_in

    @pl.when(lax.rem(lax.axis_index("cols"), 2) == 1)
    def _():
        run_copies([(ups, ups_out, PARTS), (norm, norm_out, 1)], sem)


def write_second(ups, norm, ups_out, norm_out):
    return pl.pallas_call(
        write_second_kernel,
        out_shape=[jax.ShapeDtypeStruct(a.shape, a.dtype) for a in (ups_out, norm_out)],
        in_specs=[INSIDE] * 2 + [ANYWHERE] * 2,
        out_specs=[ANYWHERE] * 2,
        input_output_aliases={2: 0, 3: 1},
        scratch_shapes=[DMA((2, PARTS))],
        compiler_params=pltpu.CompilerParams(vmem_limit_bytes=8 * MIB),
    )(ups, norm, ups_out, norm_out)


def per_device(
    n_fsdp,
    n_cols,
    train_gate,
    low_gate,
    high_gate,
    train_up,
    low_up,
    high_up,
    train_down,
    low_down,
    high_down,
    norm_train,
    norm_step,
):
    gates, ups, downs, group, norm = first(
        n_fsdp,
        n_cols,
        (train_down.T, train_gate, train_up),
        (high_down, low_gate.T, low_up.T),
        (low_down.T, high_gate, high_up),
        norm_train,
        norm_step,
    )
    gates, ups, downs, norm, group = write_first(gates, ups, downs, norm, group)
    late_ups, late_norm = second(n_fsdp, n_cols, norm_train.shape[0], train_up, low_up.T, high_up, group)
    ups, norm = write_second(late_ups, late_norm, ups, norm)
    return gates, ups, downs, norm.reshape(-1)


def solution(mesh):
    return jax.shard_map(
        functools.partial(per_device, mesh.shape["fsdp"], mesh.shape["cols"]),
        mesh=mesh,
        in_specs=(
            P("fsdp", "cols"),
            P("fsdp", None),
            P(None, "cols"),
            P("fsdp", "cols"),
            P("fsdp", None),
            P(None, "cols"),
            P("cols", "fsdp"),
            P("cols", None),
            P(None, "fsdp"),
            P(("fsdp", "cols")),
            P(("fsdp", "cols")),
        ),
        out_specs=(P(None, "cols"), P(None, "cols"), P("cols", None), P()),
        check_vma=False,
    )
```

```python
import functools

import jax
import jax.numpy as jnp
from jax import lax
from jax.experimental import pallas as pl
from jax.experimental.pallas import tpu as pltpu
from jax.sharding import PartitionSpec as P

MESH = pl.DeviceIdType.MESH
LANES = 128
DEPTH = 8
PIECES = 3
mix_rate = 1.0

ORDER = (
    (0, 0, 0, 0), (1, 0, 0, 0), (2, 0, 0, 0), (0, 0, 0, 1), (1, 0, 0, 2), (2, 0, 0, 2),
    (0, 0, 7, 0), (1, 0, 1, 0), (2, 0, 1, 0), (0, 1, 0, 0), (1, 0, 1, 2), (2, 0, 1, 2),
    (0, 0, 6, 0), (1, 0, 2, 0), (2, 0, 2, 0), (1, 0, 0, 1), (0, 1, 7, 0), (2, 0, 2, 2),
    (0, 1, 0, 2), (2, 0, 5, 0), (0, 0, 5, 0), (2, 0, 0, 1), (0, 0, 7, 1), (1, 1, 2, 0),
    (2, 0, 1, 1), (2, 0, 7, 1), (1, 1, 2, 2), (1, 1, 3, 0), (0, 1, 7, 2), (1, 1, 3, 2),
    (1, 0, 2, 2), (0, 0, 6, 1), (2, 0, 6, 1), (1, 1, 1, 1), (1, 0, 1, 1), (0, 1, 6, 2),
    (2, 1, 4, 2), (2, 1, 7, 2), (0, 1, 6, 1), (0, 0, 5, 1), (1, 1, 2, 1), (2, 1, 5, 2),
    (2, 1, 6, 2), (0, 1, 5, 1), (1, 0, 2, 1),
)
SLOTS = len(ORDER) // 3
LATE = 6
NORM_AT = (8, 10, 12)
NORM_SPREAD_AT, NORM_LAST_AT = 30, len(ORDER) - LATE - 1
WRITES = 4


def received(port, column, offset, piece):
    if port == 0:
        return column, (offset - 1) % DEPTH, piece
    if port == 1:
        return column, (offset + 1) % DEPTH, piece
    return 1 - column, offset, piece


def plan():
    arrives, slots, sends = {}, [0, 0, 0], []
    for port, *item in ORDER:
        arrives[received(port, *item)] = (port, slots[port])
        sends.append((port, slots[port], tuple(item)))
        slots[port] += 1
    return sends, arrives


def partners_of(col):
    core, x, y = lax.rem(col, 2), lax.rem(lax.div(col, 2), 4), lax.div(col, 8)
    odd = lax.rem(x, 2)

    def at(y, x, core):
        return (4 * y + x) * 2 + core

    return (
        at(y, x, 1 - core),
        at(y, x + 1 - 2 * odd, core),
        at(y, lax.rem(x + 3 + 2 * odd, 4), core),
        at(1 - y, x, core),
    )


def targets_of(here):
    place, side = lax.div(here, 2), lax.rem(here, 2)
    return (
        2 * lax.rem(place + 1, DEPTH) + side,
        2 * lax.rem(place + DEPTH - 1, DEPTH) + side,
        2 * place + 1 - side,
    )


def rows_of(item, rows):
    here = lax.axis_index("fsdp")
    place, side = lax.div(here, 2), lax.rem(here, 2)
    column, offset = item[:2]
    block = 2 * lax.rem(place + offset, DEPTH) + (side if column == 0 else 1 - side)
    return pl.ds(pl.multiple_of(block * rows, 32), rows)


def is_core(core):
    return lax.rem(lax.axis_index("cols"), 2) == core


def gather_kernel(n_fsdp, n_cols, *refs):
    bases, lows, highs = refs[0:3], refs[3:6], refs[6:9]
    norm_train, norm_step = refs[9:11]
    gates, ups, downs, serve_norm = refs[11:15]
    turned, base_vm, low_vm, high_down, high_gate, high_up, train_vm, step_vm, sums, parts, groups = refs[15:26]
    send_sem, recv_sem, local_sem, col_send, col_recv, row_send, row_recv, lead_sem = refs[26:]
    high_vm = (high_down, high_gate, high_up)
    wholes = (turned, gates, ups)
    rows = base_vm.shape[1]
    here, col = lax.axis_index("fsdp"), lax.axis_index("cols")

    loads = [
        pltpu.make_async_copy(src, dst, local_sem.at[s])
        for s, (src, dst) in enumerate(
            [p for c in range(PIECES) for p in ((bases[c], base_vm.at[c]), (lows[c], low_vm.at[c]), (highs[c], high_vm[c]))]
            + [(norm_train, train_vm), (norm_step, step_vm)]
        )
    ]
    for load in loads:
        load.start()

    barrier = pltpu.get_barrier_semaphore()
    targets = targets_of(here)
    for peer in targets:
        pl.semaphore_signal(barrier, inc=1, device_id={"fsdp": peer}, device_id_type=MESH)
    partners = partners_of(col)
    for peer in partners:
        pl.semaphore_signal(barrier, inc=1, device_id={"cols": peer}, device_id_type=MESH)

    def where(column, offset, piece):
        return wholes[piece].at[rows_of((column, offset), rows)]

    def merge(c):
        for load in loads[3 * c : 3 * c + 3]:
            load.wait()
        product = lax.dot_general(
            low_vm[c], high_vm[c][...], (((0,), (0,)), ((), ())), preferred_element_type=jnp.float32
        )
        where(0, 0, c)[...] = (base_vm[c].astype(jnp.float32) + mix_rate * product).astype(jnp.bfloat16)

    sends, arrives = plan()

    def copy(port, slot, item):
        return pltpu.make_async_remote_copy(
            src_ref=where(*item),
            dst_ref=where(*item),
            send_sem=send_sem.at[port, slot],
            recv_sem=recv_sem.at[port, slot],
            device_id={"fsdp": targets[port]},
            device_id_type=MESH,
        )

    held = set()

    def hold(item):
        if item in held:
            return
        held.add(item)
        if item[:2] == (0, 0):
            merge(item[2])
        else:
            port, slot = arrives[item]
            copy(port, slot, item).wait_recv()

    def turn(w):
        window = turned[LANES * w : LANES * (w + 1), :]
        downs[:, LANES * w : LANES * (w + 1)] = window.T

    length = train_vm.shape[0]
    span = n_cols * length
    tall = -(-(span + LANES - 1) // LANES)

    def exchange(step):
        return pltpu.make_async_remote_copy(
            src_ref=sums.at[step, pl.ds(0, tall)],
            dst_ref=parts.at[step, pl.ds(0, tall)],
            send_sem=col_send.at[step],
            recv_sem=col_recv.at[step],
            device_id={"cols": partners[step]},
            device_id_type=MESH,
        )

    def norm_step_at(step):
        if step == 0:
            loads[-2].wait()
            loads[-1].wait()
            flat = LANES * lax.broadcasted_iota(jnp.int32, (8, LANES), 0) + lax.broadcasted_iota(jnp.int32, (8, LANES), 1)
            first = lax.rem(here * span, LANES) + col * length
            tile = jnp.zeros((8, LANES), jnp.float32)
            for j in range(length):
                tile = jnp.where(flat == first + j, train_vm[j] + step_vm[j], tile)
            sums[0] = tile
        else:
            exchange(step - 1).wait()
            sums[step, 0:tall] = sums[step - 1, 0:tall] + parts[step - 1, 0:tall]
        exchange(step).start()

    def norm_copy(block, step):
        return pltpu.make_async_remote_copy(
            src_ref=groups.at[here, pl.ds(0, tall)],
            dst_ref=groups.at[block, pl.ds(0, tall)],
            send_sem=row_send.at[step],
            recv_sem=row_recv.at[step],
            device_id={"fsdp": lax.rem(here + step, n_fsdp)},
            device_id_type=MESH,
        )

    def norm_spread():
        exchange(3).wait()
        groups[here, 0:tall] = sums[3, 0:tall] + parts[3, 0:tall]
        for step in range(1, n_fsdp):
            norm_copy(here, step).start()

    def norm_last():
        for step in range(1, n_fsdp):
            norm_copy(lax.rem(here + n_fsdp - step, n_fsdp), step).wait()
        lines = serve_norm.shape[0]
        out = [None] * lines
        for g in range(n_fsdp):
            line = g * span // LANES
            for r in range(-(-(g * span % LANES + span) // LANES)):
                value = groups[g, r : r + 1, :]
                out[line + r] = value if out[line + r] is None else out[line + r] + value
        serve_norm[...] = jnp.concatenate(out, axis=0).astype(serve_norm.dtype)

    hold((0, 0, 0))
    pl.semaphore_wait(barrier, len(targets) + len(partners))

    @pl.when(is_core(0))
    def _():
        norm_step_at(0)
        pl.semaphore_wait(lead_sem, 1)

    downs_in = [item for item in arrives if item[2] == 0]
    windows = list(range(n_fsdp * rows // LANES))
    early, late = sends[:-LATE], sends[-LATE:]
    for at, (port, slot, item) in enumerate(early):
        hold(item)
        copy(port, slot, item).start()
        if at == 5:

            @pl.when(is_core(1))
            def _():
                norm_step_at(0)
                copy(*sends[0]).wait_send()
                pl.semaphore_signal(lead_sem, inc=1, device_id={"cols": partners[0]}, device_id_type=MESH)

        if at in NORM_AT:
            norm_step_at(NORM_AT.index(at) + 1)
        if at == NORM_SPREAD_AT:
            for i in downs_in:
                hold(i)
            norm_spread()
        if at == NORM_LAST_AT:
            norm_last()
        if at >= NORM_SPREAD_AT:
            for w in windows[:3]:
                turn(w)
            del windows[:3]
    for w in windows:
        turn(w)
    before = set(held)

    @pl.when(is_core(0))
    def _():
        for port, slot, item in late:
            hold(item)
            copy(port, slot, item).start()
        for item in arrives:
            hold(item)
        for each in sends:
            copy(*each).wait_send()

    held.clear()
    held.update(before)

    @pl.when(is_core(1))
    def _():
        for item in arrives:
            if item not in [received(port, *item) for port, _, item in late]:
                hold(item)
        for each in early[1:]:
            copy(*each).wait_send()


def late_kernel(gates, ups, token, arrived, send_sem, recv_sem):
    del token
    targets = targets_of(lax.axis_index("fsdp"))
    barrier = pltpu.get_barrier_semaphore()

    @pl.when(is_core(1))
    def _():
        for peer in targets:
            pl.semaphore_signal(barrier, inc=1, device_id={"fsdp": peer}, device_id_type=MESH)
        pl.semaphore_wait(barrier, len(targets))
        copies = []
        for n, (port, *item) in enumerate(ORDER[-LATE:]):
            whole = gates if item[2] == 1 else ups
            copies.append(
                pltpu.make_async_remote_copy(
                    src_ref=whole.at[rows_of(item, arrived.shape[1])],
                    dst_ref=arrived.at[n],
                    send_sem=send_sem.at[n],
                    recv_sem=recv_sem.at[n],
                    device_id={"fsdp": targets[port]},
                    device_id_type=MESH,
                )
            )
        for c in copies:
            c.start()
        for c in copies:
            c.wait()


def send_late(gates, ups, token):
    inside = pl.BlockSpec(memory_space=pltpu.VMEM)
    return pl.pallas_call(
        late_kernel,
        out_shape=pltpu.VMEM((LATE, gates.shape[0] // (2 * DEPTH), gates.shape[1]), gates.dtype),
        in_specs=[inside] * 3,
        out_specs=inside,
        scratch_shapes=[pltpu.SemaphoreType.DMA((LATE,)), pltpu.SemaphoreType.DMA((LATE,))],
        compiler_params=pltpu.CompilerParams(collective_id=1, has_side_effects=True, vmem_limit_bytes=8 * 2**20),
    )(*(pltpu.with_memory_space_constraint(a, pltpu.VMEM) for a in (gates, ups, token)))


def write_late_kernel(arrived, gates_in, ups_in, gates_out, ups_out, sem):
    del gates_in, ups_in

    @pl.when(is_core(1))
    def _():
        copies = []
        for n, (port, *item) in enumerate(ORDER[-LATE:]):
            item = received(port, *item)
            whole = gates_out if item[2] == 1 else ups_out
            copies.append(
                pltpu.make_async_copy(arrived.at[n], whole.at[rows_of(item, arrived.shape[1])], sem.at[n])
            )
        for c in copies:
            c.start()
        for c in copies:
            c.wait()


def write_late(arrived, gates, ups):
    anywhere = pl.BlockSpec(memory_space=pl.ANY)
    return pl.pallas_call(
        write_late_kernel,
        out_shape=[jax.ShapeDtypeStruct(a.shape, a.dtype) for a in (gates, ups)],
        in_specs=[pl.BlockSpec(memory_space=pltpu.VMEM), anywhere, anywhere],
        out_specs=[anywhere] * 2,
        input_output_aliases={1: 0, 2: 1},
        scratch_shapes=[pltpu.SemaphoreType.DMA((LATE,))],
        compiler_params=pltpu.CompilerParams(vmem_limit_bytes=8 * 2**20),
    )(arrived, gates, ups)


def gather(n_fsdp, n_cols, bases, lows, highs, norm_train, norm_step):
    rows, width = bases[0].shape
    rank = lows[0].shape[0]
    anywhere = pl.BlockSpec(memory_space=pl.ANY)
    inside = pl.BlockSpec(memory_space=pltpu.VMEM)
    dma = pltpu.SemaphoreType.DMA
    bf16, f32 = jnp.bfloat16, jnp.float32
    lines = n_fsdp * n_cols * norm_train.shape[0] // LANES
    return pl.pallas_call(
        functools.partial(gather_kernel, n_fsdp, n_cols),
        out_shape=[
            pltpu.VMEM((n_fsdp * rows, width), bf16),
            pltpu.VMEM((n_fsdp * rows, width), bf16),
            pltpu.VMEM((width, n_fsdp * rows), bf16),
            pltpu.VMEM((lines, LANES), bf16),
        ],
        in_specs=[anywhere] * 11,
        out_specs=[inside] * 4,
        scratch_shapes=[
            pltpu.VMEM((n_fsdp * rows, width), bf16),
            pltpu.VMEM((PIECES, rows, width), bf16),
            pltpu.VMEM((PIECES, rank, rows), bf16),
            pltpu.VMEM((rank, width), bf16),
            pltpu.VMEM((rank, width), bf16),
            pltpu.VMEM((rank, width), bf16),
            pltpu.SMEM(norm_train.shape, f32),
            pltpu.SMEM(norm_step.shape, f32),
            pltpu.VMEM((4, 8, LANES), f32),
            pltpu.VMEM((4, 8, LANES), f32),
            pltpu.VMEM((n_fsdp, 8, LANES), f32),
            dma((3, SLOTS)),
            dma((3, SLOTS)),
            dma((3 * PIECES + 2,)),
            dma((4,)),
            dma((4,)),
            dma((n_fsdp,)),
            dma((n_fsdp,)),
            pltpu.SemaphoreType.REGULAR,
        ],
        compiler_params=pltpu.CompilerParams(collective_id=0, has_side_effects=True, vmem_limit_bytes=42 * 2**20),
    )(*bases, *lows, *highs, norm_train, norm_step)


def write_kernel(*refs):
    ins, outs, token, sem = refs[:4], refs[4:8], refs[8], refs[9]
    token[...] = jnp.zeros_like(token)
    parts = sem.shape[1]
    copies = [pltpu.make_async_copy(ins[3], outs[3], sem.at[3, 0])]
    for p in range(parts):
        for a in range(3):
            rows = ins[a].shape[0] // parts
            part = pl.ds(p * rows, rows)
            copies.append(pltpu.make_async_copy(ins[a].at[part], outs[a].at[part], sem.at[a, p]))
    for c in copies:
        c.start()
    for c in copies:
        c.wait()


def write(arrays):
    return pl.pallas_call(
        write_kernel,
        out_shape=[jax.ShapeDtypeStruct(a.shape, a.dtype) for a in arrays] + [pltpu.VMEM((8, LANES), jnp.float32)],
        in_specs=[pl.BlockSpec(memory_space=pltpu.VMEM)] * 4,
        out_specs=[pl.BlockSpec(memory_space=pl.ANY)] * 4 + [pl.BlockSpec(memory_space=pltpu.VMEM)],
        scratch_shapes=[pltpu.SemaphoreType.DMA((4, WRITES))],
        compiler_params=pltpu.CompilerParams(vmem_limit_bytes=8 * 2**20),
    )(*arrays)


def per_device(
    n_fsdp,
    n_cols,
    train_gate,
    low_gate,
    high_gate,
    train_up,
    low_up,
    high_up,
    train_down,
    low_down,
    high_down,
    norm_train,
    norm_step,
):
    gates, ups, downs, norm = gather(
        n_fsdp,
        n_cols,
        (train_down.T, train_gate, train_up),
        (high_down, low_gate.T, low_up.T),
        (low_down.T, high_gate, high_up),
        norm_train,
        norm_step,
    )
    gates_out, ups_out, downs, norm, token = write((gates, ups, downs, norm))
    gates, ups = write_late(send_late(gates, ups, token), gates_out, ups_out)
    return gates, ups, downs, norm.reshape(-1)


def solution(mesh):
    return jax.shard_map(
        functools.partial(per_device, mesh.shape["fsdp"], mesh.shape["cols"]),
        mesh=mesh,
        in_specs=(
            P("fsdp", "cols"),
            P("fsdp", None),
            P(None, "cols"),
            P("fsdp", "cols"),
            P("fsdp", None),
            P(None, "cols"),
            P("cols", "fsdp"),
            P("cols", None),
            P(None, "fsdp"),
            P(("fsdp", "cols")),
            P(("fsdp", "cols")),
        ),
        out_specs=(P(None, "cols"), P(None, "cols"), P("cols", None), P()),
        check_vma=False,
    )
```

```python
import functools

import jax
import jax.numpy as jnp
from jax import lax
from jax.experimental import pallas as pl
from jax.experimental.pallas import tpu as pltpu
from jax.sharding import PartitionSpec as P

MESH = pl.DeviceIdType.MESH
LANES = 128
DEPTH = 8
PIECES = 3
mix_rate = 1.0

ORDER = (
    (0, 0, 0, 0), (1, 0, 0, 0), (2, 0, 0, 0), (0, 0, 0, 1), (1, 0, 0, 2), (2, 0, 0, 2),
    (0, 0, 7, 0), (1, 0, 1, 0), (2, 0, 1, 0), (0, 1, 0, 0), (1, 0, 1, 2), (2, 0, 1, 2),
    (0, 0, 6, 0), (1, 0, 2, 0), (2, 0, 2, 0), (1, 0, 0, 1), (0, 1, 7, 0), (2, 0, 2, 2),
    (0, 1, 0, 2), (2, 0, 5, 0), (0, 0, 5, 0), (2, 0, 0, 1), (0, 0, 7, 1), (1, 1, 2, 0),
    (2, 0, 1, 1), (2, 0, 7, 1), (1, 1, 2, 2), (1, 1, 3, 0), (0, 1, 7, 2), (1, 1, 3, 2),
    (1, 0, 2, 2), (0, 0, 6, 1), (2, 0, 6, 1), (1, 1, 1, 1), (1, 0, 1, 1), (0, 1, 6, 2),
    (2, 1, 4, 2), (2, 1, 7, 2), (0, 1, 6, 1), (0, 0, 5, 1), (1, 1, 2, 1), (2, 1, 5, 2),
    (2, 1, 6, 2), (0, 1, 5, 1), (1, 0, 2, 1),
)
SLOTS = len(ORDER) // 3
LATE = 6
NORM_AT = (8, 10, 12)
NORM_ACROSS_AT, NORM_SPREAD_AT, NORM_LAST_AT = 17, 30, len(ORDER) - LATE - 1
WRITES = 4


def received(port, column, offset, piece):
    if port == 0:
        return column, (offset - 1) % DEPTH, piece
    if port == 1:
        return column, (offset + 1) % DEPTH, piece
    return 1 - column, offset, piece


def plan():
    arrives, slots, sends = {}, [0, 0, 0], []
    for port, *item in ORDER:
        arrives[received(port, *item)] = (port, slots[port])
        sends.append((port, slots[port], tuple(item)))
        slots[port] += 1
    return sends, arrives


def partners_of(col):
    core, x, y = lax.rem(col, 2), lax.rem(lax.div(col, 2), 4), lax.div(col, 8)
    odd = lax.rem(x, 2)

    def at(y, x, core):
        return (4 * y + x) * 2 + core

    return (
        at(y, x, 1 - core),
        at(y, x + 1 - 2 * odd, core),
        at(y, lax.rem(x + 3 + 2 * odd, 4), core),
        at(1 - y, x, core),
    )


def targets_of(here):
    place, side = lax.div(here, 2), lax.rem(here, 2)
    return (
        2 * lax.rem(place + 1, DEPTH) + side,
        2 * lax.rem(place + DEPTH - 1, DEPTH) + side,
        2 * place + 1 - side,
    )


def rows_of(item, rows):
    here = lax.axis_index("fsdp")
    place, side = lax.div(here, 2), lax.rem(here, 2)
    column, offset = item[:2]
    block = 2 * lax.rem(place + offset, DEPTH) + (side if column == 0 else 1 - side)
    return pl.ds(pl.multiple_of(block * rows, 32), rows)


def is_core(core):
    return lax.rem(lax.axis_index("cols"), 2) == core


def gather_kernel(n_fsdp, n_cols, *refs):
    bases, lows, highs = refs[0:3], refs[3:6], refs[6:9]
    norm_train, norm_step = refs[9:11]
    gates, ups, downs, serve_norm = refs[11:15]
    turned, base_vm, low_vm, high_down, high_gate, high_up, train_vm, step_vm, sums, parts, groups = refs[15:26]
    send_sem, recv_sem, local_sem, col_send, col_recv, row_send, row_recv, lead_sem = refs[26:]
    high_vm = (high_down, high_gate, high_up)
    wholes = (turned, gates, ups)
    rows = base_vm.shape[1]
    here, col = lax.axis_index("fsdp"), lax.axis_index("cols")

    loads = [
        pltpu.make_async_copy(src, dst, local_sem.at[s])
        for s, (src, dst) in enumerate(
            [p for c in range(PIECES) for p in ((bases[c], base_vm.at[c]), (lows[c], low_vm.at[c]), (highs[c], high_vm[c]))]
            + [(norm_train, train_vm), (norm_step, step_vm)]
        )
    ]
    barrier = pltpu.get_barrier_semaphore()
    targets = targets_of(here)
    for peer in targets:
        pl.semaphore_signal(barrier, inc=1, device_id={"fsdp": peer}, device_id_type=MESH)
    partners = partners_of(col)
    for peer in partners:
        pl.semaphore_signal(barrier, inc=1, device_id={"cols": peer}, device_id_type=MESH)
    for load in loads:
        load.start()

    def where(column, offset, piece):
        return wholes[piece].at[rows_of((column, offset), rows)]

    def merge(c):
        for load in loads[3 * c : 3 * c + 3]:
            load.wait()
        product = lax.dot_general(
            low_vm[c], high_vm[c][...], (((0,), (0,)), ((), ())), preferred_element_type=jnp.float32
        )
        where(0, 0, c)[...] = (base_vm[c].astype(jnp.float32) + mix_rate * product).astype(jnp.bfloat16)

    sends, arrives = plan()

    def copy(port, slot, item):
        return pltpu.make_async_remote_copy(
            src_ref=where(*item),
            dst_ref=where(*item),
            send_sem=send_sem.at[port, slot],
            recv_sem=recv_sem.at[port, slot],
            device_id={"fsdp": targets[port]},
            device_id_type=MESH,
        )

    held = set()

    def hold(item):
        if item in held:
            return
        held.add(item)
        if item[:2] == (0, 0):
            merge(item[2])
        else:
            port, slot = arrives[item]
            copy(port, slot, item).wait_recv()

    def turn(w):
        window = turned[LANES * w : LANES * (w + 1), :]
        downs[:, LANES * w : LANES * (w + 1)] = window.T

    length = train_vm.shape[0]
    span = n_cols * length
    tall = -(-(span + LANES - 1) // LANES)

    def exchange(step):
        return pltpu.make_async_remote_copy(
            src_ref=sums.at[step, pl.ds(0, tall)],
            dst_ref=parts.at[step, pl.ds(0, tall)],
            send_sem=col_send.at[step],
            recv_sem=col_recv.at[step],
            device_id={"cols": partners[step]},
            device_id_type=MESH,
        )

    def norm_step_at(step):
        if step == 0:
            loads[-2].wait()
            loads[-1].wait()
            flat = LANES * lax.broadcasted_iota(jnp.int32, (8, LANES), 0) + lax.broadcasted_iota(jnp.int32, (8, LANES), 1)
            first = lax.rem(here * span, LANES) + col * length
            tile = jnp.zeros((8, LANES), jnp.float32)
            for j in range(length):
                tile = jnp.where(flat == first + j, train_vm[j] + step_vm[j], tile)
            sums[0] = tile
        else:
            exchange(step - 1).wait()
            sums[step, 0:tall] = sums[step - 1, 0:tall] + parts[step - 1, 0:tall]
        exchange(step).start()

    place, side = lax.div(here, 2), lax.rem(here, 2)

    def across(block):
        return pltpu.make_async_remote_copy(
            src_ref=groups.at[here, pl.ds(0, tall)],
            dst_ref=groups.at[block, pl.ds(0, tall)],
            send_sem=row_send.at[0],
            recv_sem=row_recv.at[0],
            device_id={"fsdp": targets[2]},
            device_id_type=MESH,
        )

    def along(start, step):
        return pltpu.make_async_remote_copy(
            src_ref=groups.at[pl.ds(2 * place, 2), pl.ds(0, tall)],
            dst_ref=groups.at[pl.ds(2 * start, 2), pl.ds(0, tall)],
            send_sem=row_send.at[step],
            recv_sem=row_recv.at[step],
            device_id={"fsdp": 2 * lax.rem(place + step, DEPTH) + side},
            device_id_type=MESH,
        )

    def norm_across():
        exchange(3).wait()
        groups[here, 0:tall] = sums[3, 0:tall] + parts[3, 0:tall]
        across(here).start()

    def norm_spread():
        across(2 * place + 1 - side).wait()
        for step in range(1, DEPTH):
            along(place, step).start()

    def norm_last():
        for step in range(1, DEPTH):
            along(lax.rem(place + DEPTH - step, DEPTH), step).wait()
        lines = serve_norm.shape[0]
        out = [None] * lines
        for g in range(n_fsdp):
            line = g * span // LANES
            for r in range(-(-(g * span % LANES + span) // LANES)):
                value = groups[g, r : r + 1, :]
                out[line + r] = value if out[line + r] is None else out[line + r] + value
        serve_norm[...] = jnp.concatenate(out, axis=0).astype(serve_norm.dtype)

    hold((0, 0, 0))
    pl.semaphore_wait(barrier, len(targets) + len(partners))

    @pl.when(is_core(0))
    def _():
        norm_step_at(0)
        pl.semaphore_wait(lead_sem, 1)

    downs_in = [item for item in arrives if item[2] == 0]
    windows = list(range(n_fsdp * rows // LANES))
    early, late = sends[:-LATE], sends[-LATE:]
    for at, (port, slot, item) in enumerate(early):
        hold(item)
        copy(port, slot, item).start()
        if at == 5:

            @pl.when(is_core(1))
            def _():
                norm_step_at(0)
                copy(*sends[0]).wait_send()
                pl.semaphore_signal(lead_sem, inc=1, device_id={"cols": partners[0]}, device_id_type=MESH)

        if at in NORM_AT:
            norm_step_at(NORM_AT.index(at) + 1)
        if at == NORM_ACROSS_AT:
            norm_across()
        if at == NORM_SPREAD_AT:
            for i in downs_in:
                hold(i)
            norm_spread()
        if at == NORM_LAST_AT:
            norm_last()
        if at >= NORM_SPREAD_AT:
            for w in windows[:3]:
                turn(w)
            del windows[:3]
    for w in windows:
        turn(w)
    before = set(held)

    @pl.when(is_core(0))
    def _():
        for port, slot, item in late:
            hold(item)
            copy(port, slot, item).start()
        for item in arrives:
            hold(item)
        for each in sends:
            copy(*each).wait_send()

    held.clear()
    held.update(before)

    @pl.when(is_core(1))
    def _():
        for item in arrives:
            if item not in [received(port, *item) for port, _, item in late]:
                hold(item)
        for each in early[1:]:
            copy(*each).wait_send()


def late_kernel(gates, ups, token, arrived, send_sem, recv_sem):
    del token
    targets = targets_of(lax.axis_index("fsdp"))
    barrier = pltpu.get_barrier_semaphore()

    @pl.when(is_core(1))
    def _():
        for peer in targets:
            pl.semaphore_signal(barrier, inc=1, device_id={"fsdp": peer}, device_id_type=MESH)
        pl.semaphore_wait(barrier, len(targets))
        copies = []
        for n, (port, *item) in enumerate(ORDER[-LATE:]):
            whole = gates if item[2] == 1 else ups
            copies.append(
                pltpu.make_async_remote_copy(
                    src_ref=whole.at[rows_of(item, arrived.shape[1])],
                    dst_ref=arrived.at[n],
                    send_sem=send_sem.at[n],
                    recv_sem=recv_sem.at[n],
                    device_id={"fsdp": targets[port]},
                    device_id_type=MESH,
                )
            )
        for c in copies:
            c.start()
        for c in copies:
            c.wait()


def send_late(gates, ups, token):
    inside = pl.BlockSpec(memory_space=pltpu.VMEM)
    return pl.pallas_call(
        late_kernel,
        out_shape=pltpu.VMEM((LATE, gates.shape[0] // (2 * DEPTH), gates.shape[1]), gates.dtype),
        in_specs=[inside] * 3,
        out_specs=inside,
        scratch_shapes=[pltpu.SemaphoreType.DMA((LATE,)), pltpu.SemaphoreType.DMA((LATE,))],
        compiler_params=pltpu.CompilerParams(collective_id=1, has_side_effects=True, vmem_limit_bytes=8 * 2**20),
    )(*(pltpu.with_memory_space_constraint(a, pltpu.VMEM) for a in (gates, ups, token)))


def write_late_kernel(arrived, gates_in, ups_in, gates_out, ups_out, sem):
    del gates_in, ups_in

    @pl.when(is_core(1))
    def _():
        copies = []
        for n, (port, *item) in enumerate(ORDER[-LATE:]):
            item = received(port, *item)
            whole = gates_out if item[2] == 1 else ups_out
            copies.append(
                pltpu.make_async_copy(arrived.at[n], whole.at[rows_of(item, arrived.shape[1])], sem.at[n])
            )
        for c in copies:
            c.start()
        for c in copies:
            c.wait()


def write_late(arrived, gates, ups):
    anywhere = pl.BlockSpec(memory_space=pl.ANY)
    return pl.pallas_call(
        write_late_kernel,
        out_shape=[jax.ShapeDtypeStruct(a.shape, a.dtype) for a in (gates, ups)],
        in_specs=[pl.BlockSpec(memory_space=pltpu.VMEM), anywhere, anywhere],
        out_specs=[anywhere] * 2,
        input_output_aliases={1: 0, 2: 1},
        scratch_shapes=[pltpu.SemaphoreType.DMA((LATE,))],
        compiler_params=pltpu.CompilerParams(vmem_limit_bytes=8 * 2**20),
    )(arrived, gates, ups)


def gather(n_fsdp, n_cols, bases, lows, highs, norm_train, norm_step):
    rows, width = bases[0].shape
    rank = lows[0].shape[0]
    anywhere = pl.BlockSpec(memory_space=pl.ANY)
    inside = pl.BlockSpec(memory_space=pltpu.VMEM)
    dma = pltpu.SemaphoreType.DMA
    bf16, f32 = jnp.bfloat16, jnp.float32
    lines = n_fsdp * n_cols * norm_train.shape[0] // LANES
    return pl.pallas_call(
        functools.partial(gather_kernel, n_fsdp, n_cols),
        out_shape=[
            pltpu.VMEM((n_fsdp * rows, width), bf16),
            pltpu.VMEM((n_fsdp * rows, width), bf16),
            pltpu.VMEM((width, n_fsdp * rows), bf16),
            pltpu.VMEM((lines, LANES), bf16),
        ],
        in_specs=[anywhere] * 11,
        out_specs=[inside] * 4,
        scratch_shapes=[
            pltpu.VMEM((n_fsdp * rows, width), bf16),
            pltpu.VMEM((PIECES, rows, width), bf16),
            pltpu.VMEM((PIECES, rank, rows), bf16),
            pltpu.VMEM((rank, width), bf16),
            pltpu.VMEM((rank, width), bf16),
            pltpu.VMEM((rank, width), bf16),
            pltpu.SMEM(norm_train.shape, f32),
            pltpu.SMEM(norm_step.shape, f32),
            pltpu.VMEM((4, 8, LANES), f32),
            pltpu.VMEM((4, 8, LANES), f32),
            pltpu.VMEM((n_fsdp, 8, LANES), f32),
            dma((3, SLOTS)),
            dma((3, SLOTS)),
            dma((3 * PIECES + 2,)),
            dma((4,)),
            dma((4,)),
            dma((DEPTH,)),
            dma((DEPTH,)),
            pltpu.SemaphoreType.REGULAR,
        ],
        compiler_params=pltpu.CompilerParams(collective_id=0, has_side_effects=True, vmem_limit_bytes=42 * 2**20),
    )(*bases, *lows, *highs, norm_train, norm_step)


def write_kernel(*refs):
    ins, outs, token, sem = refs[:4], refs[4:8], refs[8], refs[9]
    token[...] = jnp.zeros_like(token)
    parts = sem.shape[1]
    copies = [pltpu.make_async_copy(ins[3], outs[3], sem.at[3, 0])]
    for p in range(parts):
        for a in range(3):
            rows = ins[a].shape[0] // parts
            part = pl.ds(p * rows, rows)
            copies.append(pltpu.make_async_copy(ins[a].at[part], outs[a].at[part], sem.at[a, p]))
    for c in copies:
        c.start()
    for c in copies:
        c.wait()


def write(arrays):
    return pl.pallas_call(
        write_kernel,
        out_shape=[jax.ShapeDtypeStruct(a.shape, a.dtype) for a in arrays] + [pltpu.VMEM((8, LANES), jnp.float32)],
        in_specs=[pl.BlockSpec(memory_space=pltpu.VMEM)] * 4,
        out_specs=[pl.BlockSpec(memory_space=pl.ANY)] * 4 + [pl.BlockSpec(memory_space=pltpu.VMEM)],
        scratch_shapes=[pltpu.SemaphoreType.DMA((4, WRITES))],
        compiler_params=pltpu.CompilerParams(vmem_limit_bytes=8 * 2**20),
    )(*arrays)


def per_device(
    n_fsdp,
    n_cols,
    train_gate,
    low_gate,
    high_gate,
    train_up,
    low_up,
    high_up,
    train_down,
    low_down,
    high_down,
    norm_train,
    norm_step,
):
    gates, ups, downs, norm = gather(
        n_fsdp,
        n_cols,
        (train_down.T, train_gate, train_up),
        (high_down, low_gate.T, low_up.T),
        (low_down.T, high_gate, high_up),
        norm_train,
        norm_step,
    )
    gates_out, ups_out, downs, norm, token = write((gates, ups, downs, norm))
    gates, ups = write_late(send_late(gates, ups, token), gates_out, ups_out)
    return gates, ups, downs, norm.reshape(-1)


def solution(mesh):
    return jax.shard_map(
        functools.partial(per_device, mesh.shape["fsdp"], mesh.shape["cols"]),
        mesh=mesh,
        in_specs=(
            P("fsdp", "cols"),
            P("fsdp", None),
            P(None, "cols"),
            P("fsdp", "cols"),
            P("fsdp", None),
            P(None, "cols"),
            P("cols", "fsdp"),
            P("cols", None),
            P(None, "fsdp"),
            P(("fsdp", "cols")),
            P(("fsdp", "cols")),
        ),
        out_specs=(P(None, "cols"), P(None, "cols"), P("cols", None), P()),
        check_vma=False,
    )
```

```python
import functools

import jax
import jax.numpy as jnp
from jax import lax
from jax.experimental import pallas as pl
from jax.experimental.pallas import tpu as pltpu
from jax.sharding import PartitionSpec as P

MESH = pl.DeviceIdType.MESH
LANES = 128
DEPTH = 8
PIECES = 3
mix_rate = 1.0

ORDER = (
    (0, 0, 0, 0), (1, 0, 0, 0), (2, 0, 0, 0), (0, 0, 0, 1), (1, 0, 0, 2), (2, 0, 0, 2),
    (0, 0, 7, 0), (1, 0, 1, 0), (2, 0, 1, 0), (0, 1, 0, 0), (1, 0, 1, 2), (2, 0, 1, 2),
    (0, 0, 6, 0), (1, 0, 2, 0), (2, 0, 2, 0), (1, 0, 0, 1), (0, 1, 7, 0), (2, 0, 2, 2),
    (0, 1, 0, 2), (2, 0, 5, 0), (0, 0, 5, 0), (2, 0, 0, 1), (0, 0, 7, 1), (1, 1, 2, 0),
    (2, 0, 1, 1), (2, 0, 7, 1), (1, 1, 2, 2), (1, 1, 3, 0), (0, 1, 7, 2), (1, 1, 3, 2),
    (1, 0, 2, 2), (0, 0, 6, 1), (2, 0, 6, 1), (1, 1, 1, 1), (1, 0, 1, 1), (0, 1, 6, 2),
    (2, 1, 4, 2), (2, 1, 7, 2), (0, 1, 6, 1), (0, 0, 5, 1), (1, 1, 2, 1), (2, 1, 5, 2),
    (2, 1, 6, 2), (0, 1, 5, 1), (1, 0, 2, 1),
)
SLOTS = len(ORDER) // 3
LATE = 6
NORM_AT = (8, 10, 12)
NORM_ACROSS_AT, NORM_SPREAD_AT, NORM_LAST_AT = 17, 30, len(ORDER) - LATE - 1
WRITES = 4


def received(port, column, offset, piece):
    if port == 0:
        return column, (offset - 1) % DEPTH, piece
    if port == 1:
        return column, (offset + 1) % DEPTH, piece
    return 1 - column, offset, piece


def plan():
    arrives, slots, sends = {}, [0, 0, 0], []
    for port, *item in ORDER:
        arrives[received(port, *item)] = (port, slots[port])
        sends.append((port, slots[port], tuple(item)))
        slots[port] += 1
    return sends, arrives


def partners_of(col):
    core, x, y = lax.rem(col, 2), lax.rem(lax.div(col, 2), 4), lax.div(col, 8)
    odd = lax.rem(x, 2)

    def at(y, x, core):
        return (4 * y + x) * 2 + core

    return (
        at(y, x, 1 - core),
        at(y, x + 1 - 2 * odd, core),
        at(y, lax.rem(x + 3 + 2 * odd, 4), core),
        at(1 - y, x, core),
    )


def targets_of(here):
    place, side = lax.div(here, 2), lax.rem(here, 2)
    return (
        2 * lax.rem(place + 1, DEPTH) + side,
        2 * lax.rem(place + DEPTH - 1, DEPTH) + side,
        2 * place + 1 - side,
    )


def rows_of(item, rows):
    here = lax.axis_index("fsdp")
    place, side = lax.div(here, 2), lax.rem(here, 2)
    column, offset = item[:2]
    block = 2 * lax.rem(place + offset, DEPTH) + (side if column == 0 else 1 - side)
    return pl.ds(pl.multiple_of(block * rows, 32), rows)


def is_core(core):
    return lax.rem(lax.axis_index("cols"), 2) == core


def gather_kernel(n_fsdp, n_cols, *refs):
    bases, lows, highs = refs[0:3], refs[3:6], refs[6:9]
    norm_train, norm_step = refs[9:11]
    gates, ups, downs, serve_norm = refs[11:15]
    turned, base_vm, low_vm, high_down, high_gate, high_up, train_vm, step_vm, sums, parts, groups = refs[15:26]
    send_sem, recv_sem, local_sem, col_send, col_recv, row_send, row_recv, lead_sem = refs[26:]
    high_vm = (high_down, high_gate, high_up)
    wholes = (turned, gates, ups)
    rows = base_vm.shape[1]
    here, col = lax.axis_index("fsdp"), lax.axis_index("cols")

    loads = [
        pltpu.make_async_copy(src, dst, local_sem.at[s])
        for s, (src, dst) in enumerate(
            [p for c in range(PIECES) for p in ((bases[c], base_vm.at[c]), (lows[c], low_vm.at[c]), (highs[c], high_vm[c]))]
            + [(norm_train, train_vm), (norm_step, step_vm)]
        )
    ]
    barrier = pltpu.get_barrier_semaphore()
    targets = targets_of(here)
    for peer in targets:
        pl.semaphore_signal(barrier, inc=1, device_id={"fsdp": peer}, device_id_type=MESH)
    partners = partners_of(col)
    for peer in partners:
        pl.semaphore_signal(barrier, inc=1, device_id={"cols": peer}, device_id_type=MESH)
    for load in loads[:3]:
        load.start()

    def where(column, offset, piece):
        return wholes[piece].at[rows_of((column, offset), rows)]

    def merge(c):
        for load in loads[3 * c : 3 * c + 3]:
            load.wait()
        if c == 0:
            for load in loads[3:]:
                load.start()
        product = lax.dot_general(
            low_vm[c], high_vm[c][...], (((0,), (0,)), ((), ())), preferred_element_type=jnp.float32
        )
        where(0, 0, c)[...] = (base_vm[c].astype(jnp.float32) + mix_rate * product).astype(jnp.bfloat16)

    sends, arrives = plan()

    def copy(port, slot, item):
        return pltpu.make_async_remote_copy(
            src_ref=where(*item),
            dst_ref=where(*item),
            send_sem=send_sem.at[port, slot],
            recv_sem=recv_sem.at[port, slot],
            device_id={"fsdp": targets[port]},
            device_id_type=MESH,
        )

    held = set()

    def hold(item):
        if item in held:
            return
        held.add(item)
        if item[:2] == (0, 0):
            merge(item[2])
        else:
            port, slot = arrives[item]
            copy(port, slot, item).wait_recv()

    def turn(w):
        window = turned[LANES * w : LANES * (w + 1), :]
        downs[:, LANES * w : LANES * (w + 1)] = window.T

    length = train_vm.shape[0]
    span = n_cols * length
    tall = -(-(span + LANES - 1) // LANES)

    def exchange(step):
        return pltpu.make_async_remote_copy(
            src_ref=sums.at[step, pl.ds(0, tall)],
            dst_ref=parts.at[step, pl.ds(0, tall)],
            send_sem=col_send.at[step],
            recv_sem=col_recv.at[step],
            device_id={"cols": partners[step]},
            device_id_type=MESH,
        )

    def norm_step_at(step):
        if step == 0:
            loads[-2].wait()
            loads[-1].wait()
            flat = LANES * lax.broadcasted_iota(jnp.int32, (8, LANES), 0) + lax.broadcasted_iota(jnp.int32, (8, LANES), 1)
            first = lax.rem(here * span, LANES) + col * length
            tile = jnp.zeros((8, LANES), jnp.float32)
            for j in range(length):
                tile = jnp.where(flat == first + j, train_vm[j] + step_vm[j], tile)
            sums[0] = tile
        else:
            exchange(step - 1).wait()
            sums[step, 0:tall] = sums[step - 1, 0:tall] + parts[step - 1, 0:tall]
        exchange(step).start()

    place, side = lax.div(here, 2), lax.rem(here, 2)

    def across(block):
        return pltpu.make_async_remote_copy(
            src_ref=groups.at[here, pl.ds(0, tall)],
            dst_ref=groups.at[block, pl.ds(0, tall)],
            send_sem=row_send.at[0],
            recv_sem=row_recv.at[0],
            device_id={"fsdp": targets[2]},
            device_id_type=MESH,
        )

    def along(start, step):
        return pltpu.make_async_remote_copy(
            src_ref=groups.at[pl.ds(2 * place, 2), pl.ds(0, tall)],
            dst_ref=groups.at[pl.ds(2 * start, 2), pl.ds(0, tall)],
            send_sem=row_send.at[step],
            recv_sem=row_recv.at[step],
            device_id={"fsdp": 2 * lax.rem(place + step, DEPTH) + side},
            device_id_type=MESH,
        )

    def norm_across():
        exchange(3).wait()
        groups[here, 0:tall] = sums[3, 0:tall] + parts[3, 0:tall]
        across(here).start()

    def norm_spread():
        across(2 * place + 1 - side).wait()
        for step in range(1, DEPTH):
            along(place, step).start()

    def norm_last():
        for step in range(1, DEPTH):
            along(lax.rem(place + DEPTH - step, DEPTH), step).wait()
        lines = serve_norm.shape[0]
        out = [None] * lines
        for g in range(n_fsdp):
            line = g * span // LANES
            for r in range(-(-(g * span % LANES + span) // LANES)):
                value = groups[g, r : r + 1, :]
                out[line + r] = value if out[line + r] is None else out[line + r] + value
        serve_norm[...] = jnp.concatenate(out, axis=0).astype(serve_norm.dtype)

    hold((0, 0, 0))
    pl.semaphore_wait(barrier, len(targets) + len(partners))

    @pl.when(is_core(0))
    def _():
        norm_step_at(0)
        pl.semaphore_wait(lead_sem, 1)

    downs_in = [item for item in arrives if item[2] == 0]
    windows = list(range(n_fsdp * rows // LANES))
    early, late = sends[:-LATE], sends[-LATE:]
    for at, (port, slot, item) in enumerate(early):
        hold(item)
        copy(port, slot, item).start()
        if at == 5:

            @pl.when(is_core(1))
            def _():
                norm_step_at(0)
                copy(*sends[0]).wait_send()
                pl.semaphore_signal(lead_sem, inc=1, device_id={"cols": partners[0]}, device_id_type=MESH)

        if at in NORM_AT:
            norm_step_at(NORM_AT.index(at) + 1)
        if at == NORM_ACROSS_AT:
            norm_across()
        if at == NORM_SPREAD_AT:
            for i in downs_in:
                hold(i)
            norm_spread()
        if at == NORM_LAST_AT:
            norm_last()
        if at >= NORM_SPREAD_AT:
            for w in windows[:3]:
                turn(w)
            del windows[:3]
    for w in windows:
        turn(w)
    before = set(held)

    @pl.when(is_core(0))
    def _():
        for port, slot, item in late:
            hold(item)
            copy(port, slot, item).start()
        for item in arrives:
            hold(item)
        for each in sends:
            copy(*each).wait_send()

    held.clear()
    held.update(before)

    @pl.when(is_core(1))
    def _():
        for item in arrives:
            if item not in [received(port, *item) for port, _, item in late]:
                hold(item)
        for each in early[1:]:
            copy(*each).wait_send()


def late_kernel(gates, ups, token, arrived, send_sem, recv_sem):
    del token
    targets = targets_of(lax.axis_index("fsdp"))
    barrier = pltpu.get_barrier_semaphore()

    @pl.when(is_core(1))
    def _():
        for peer in targets:
            pl.semaphore_signal(barrier, inc=1, device_id={"fsdp": peer}, device_id_type=MESH)
        pl.semaphore_wait(barrier, len(targets))
        copies = []
        for n, (port, *item) in enumerate(ORDER[-LATE:]):
            whole = gates if item[2] == 1 else ups
            copies.append(
                pltpu.make_async_remote_copy(
                    src_ref=whole.at[rows_of(item, arrived.shape[1])],
                    dst_ref=arrived.at[n],
                    send_sem=send_sem.at[n],
                    recv_sem=recv_sem.at[n],
                    device_id={"fsdp": targets[port]},
                    device_id_type=MESH,
                )
            )
        for c in copies:
            c.start()
        for c in copies:
            c.wait()


def send_late(gates, ups, token):
    inside = pl.BlockSpec(memory_space=pltpu.VMEM)
    return pl.pallas_call(
        late_kernel,
        out_shape=pltpu.VMEM((LATE, gates.shape[0] // (2 * DEPTH), gates.shape[1]), gates.dtype),
        in_specs=[inside] * 3,
        out_specs=inside,
        scratch_shapes=[pltpu.SemaphoreType.DMA((LATE,)), pltpu.SemaphoreType.DMA((LATE,))],
        compiler_params=pltpu.CompilerParams(collective_id=1, has_side_effects=True, vmem_limit_bytes=8 * 2**20),
    )(*(pltpu.with_memory_space_constraint(a, pltpu.VMEM) for a in (gates, ups, token)))


def write_late_kernel(arrived, gates_in, ups_in, gates_out, ups_out, sem):
    del gates_in, ups_in

    @pl.when(is_core(1))
    def _():
        copies = []
        for n, (port, *item) in enumerate(ORDER[-LATE:]):
            item = received(port, *item)
            whole = gates_out if item[2] == 1 else ups_out
            copies.append(
                pltpu.make_async_copy(arrived.at[n], whole.at[rows_of(item, arrived.shape[1])], sem.at[n])
            )
        for c in copies:
            c.start()
        for c in copies:
            c.wait()


def write_late(arrived, gates, ups):
    anywhere = pl.BlockSpec(memory_space=pl.ANY)
    return pl.pallas_call(
        write_late_kernel,
        out_shape=[jax.ShapeDtypeStruct(a.shape, a.dtype) for a in (gates, ups)],
        in_specs=[pl.BlockSpec(memory_space=pltpu.VMEM), anywhere, anywhere],
        out_specs=[anywhere] * 2,
        input_output_aliases={1: 0, 2: 1},
        scratch_shapes=[pltpu.SemaphoreType.DMA((LATE,))],
        compiler_params=pltpu.CompilerParams(vmem_limit_bytes=8 * 2**20),
    )(arrived, gates, ups)


def gather(n_fsdp, n_cols, bases, lows, highs, norm_train, norm_step):
    rows, width = bases[0].shape
    rank = lows[0].shape[0]
    anywhere = pl.BlockSpec(memory_space=pl.ANY)
    inside = pl.BlockSpec(memory_space=pltpu.VMEM)
    dma = pltpu.SemaphoreType.DMA
    bf16, f32 = jnp.bfloat16, jnp.float32
    lines = n_fsdp * n_cols * norm_train.shape[0] // LANES
    return pl.pallas_call(
        functools.partial(gather_kernel, n_fsdp, n_cols),
        out_shape=[
            pltpu.VMEM((n_fsdp * rows, width), bf16),
            pltpu.VMEM((n_fsdp * rows, width), bf16),
            pltpu.VMEM((width, n_fsdp * rows), bf16),
            pltpu.VMEM((lines, LANES), bf16),
        ],
        in_specs=[anywhere] * 11,
        out_specs=[inside] * 4,
        scratch_shapes=[
            pltpu.VMEM((n_fsdp * rows, width), bf16),
            pltpu.VMEM((PIECES, rows, width), bf16),
            pltpu.VMEM((PIECES, rank, rows), bf16),
            pltpu.VMEM((rank, width), bf16),
            pltpu.VMEM((rank, width), bf16),
            pltpu.VMEM((rank, width), bf16),
            pltpu.SMEM(norm_train.shape, f32),
            pltpu.SMEM(norm_step.shape, f32),
            pltpu.VMEM((4, 8, LANES), f32),
            pltpu.VMEM((4, 8, LANES), f32),
            pltpu.VMEM((n_fsdp, 8, LANES), f32),
            dma((3, SLOTS)),
            dma((3, SLOTS)),
            dma((3 * PIECES + 2,)),
            dma((4,)),
            dma((4,)),
            dma((DEPTH,)),
            dma((DEPTH,)),
            pltpu.SemaphoreType.REGULAR,
        ],
        compiler_params=pltpu.CompilerParams(collective_id=0, has_side_effects=True, vmem_limit_bytes=42 * 2**20),
    )(*bases, *lows, *highs, norm_train, norm_step)


def write_kernel(*refs):
    ins, outs, token, sem = refs[:4], refs[4:8], refs[8], refs[9]
    token[...] = jnp.zeros_like(token)
    parts = sem.shape[1]
    copies = [pltpu.make_async_copy(ins[3], outs[3], sem.at[3, 0])]
    for p in range(parts):
        for a in range(3):
            rows = ins[a].shape[0] // parts
            part = pl.ds(p * rows, rows)
            copies.append(pltpu.make_async_copy(ins[a].at[part], outs[a].at[part], sem.at[a, p]))
    for c in copies:
        c.start()
    for c in copies:
        c.wait()


def write(arrays):
    return pl.pallas_call(
        write_kernel,
        out_shape=[jax.ShapeDtypeStruct(a.shape, a.dtype) for a in arrays] + [pltpu.VMEM((8, LANES), jnp.float32)],
        in_specs=[pl.BlockSpec(memory_space=pltpu.VMEM)] * 4,
        out_specs=[pl.BlockSpec(memory_space=pl.ANY)] * 4 + [pl.BlockSpec(memory_space=pltpu.VMEM)],
        scratch_shapes=[pltpu.SemaphoreType.DMA((4, WRITES))],
        compiler_params=pltpu.CompilerParams(vmem_limit_bytes=8 * 2**20),
    )(*arrays)


def per_device(
    n_fsdp,
    n_cols,
    train_gate,
    low_gate,
    high_gate,
    train_up,
    low_up,
    high_up,
    train_down,
    low_down,
    high_down,
    norm_train,
    norm_step,
):
    gates, ups, downs, norm = gather(
        n_fsdp,
        n_cols,
        (train_down.T, train_gate, train_up),
        (high_down, low_gate.T, low_up.T),
        (low_down.T, high_gate, high_up),
        norm_train,
        norm_step,
    )
    gates_out, ups_out, downs, norm, token = write((gates, ups, downs, norm))
    gates, ups = write_late(send_late(gates, ups, token), gates_out, ups_out)
    return gates, ups, downs, norm.reshape(-1)


def solution(mesh):
    return jax.shard_map(
        functools.partial(per_device, mesh.shape["fsdp"], mesh.shape["cols"]),
        mesh=mesh,
        in_specs=(
            P("fsdp", "cols"),
            P("fsdp", None),
            P(None, "cols"),
            P("fsdp", "cols"),
            P("fsdp", None),
            P(None, "cols"),
            P("cols", "fsdp"),
            P("cols", None),
            P(None, "fsdp"),
            P(("fsdp", "cols")),
            P(("fsdp", "cols")),
        ),
        out_specs=(P(None, "cols"), P(None, "cols"), P("cols", None), P()),
        check_vma=False,
    )
```
